256 devices in a mesh: pipe: 8 (over x, z_lo), tensor: 4 (over y), expert: 8 (over z_hi, core).
Axes of the slice: x: 4, y: 4, z: 8 (z_hi: 4, z_lo: 2; z = z_hi * 2 + z_lo), core: 2. Of those that a mesh axis runs over, the one named last changes fastest.
Arguments:
- tokens: bfloat16 [2, 512, 4096], P(None, 'expert'), may hold values from -6 to 6
- gains: float32 [8, 4096], P('pipe'), may hold values from 0.1 to 1.9
- route_ids: int32 [8, 2, 512, 2], P('pipe', None, 'expert'), may hold values from 0 to 7, all different within a row
- route_weights: float32 [8, 2, 512, 2], P('pipe', None, 'expert'), may hold values from 0.2 to 1
- picks: int32 [8, 2, 8, 64], P('pipe', None, 'expert'), may hold values from 0 to 63, each once within a row
- w_gate: bfloat16 [8, 8, 4096, 1536], P('pipe', 'expert', None, 'tensor'), may hold values from -0.09375 to 0.09375
- w_up: bfloat16 [8, 8, 4096, 1536], P('pipe', 'expert', None, 'tensor'), may hold values from -0.09375 to 0.09375
- w_down: bfloat16 [8, 8, 1536, 4096], P('pipe', 'expert', 'tensor'), may hold values from -0.15625 to 0.15625
Outputs:
- streams: bfloat16 [8, 2, 512, 4096], P('pipe', None, 'expert', 'tensor')
The draws below stay inside these ranges and needn't reach their ends.
Inputs may be any that keep to these rules, and one draw needn't show every extreme that they name: `route_ids`: each token names 2 different experts; every expert is named by some token. `picks`: for every layer, micro-batch and block of 64 tokens, a permutation of 0 to 63.
All inputs are finite; a program needn't handle non-finite values.
Results may differ from the reference program's by a relative error of at most 0.025.
Values may be sent and summed in bfloat16 or wider, within the bound.
No kernel may reach another device: no remote copies, remote signals or barrier semaphores. Data moves between devices by JAX's collectives and lax.ppermute only.
A program may use at most 64 MiB of HBM per device.

```python
import jax
import jax.numpy as jnp
from jax import lax

D = 4096
FF = 1536
TOPK = 2
MICRO = 2
TOK_DEV = 64
EXPERTS = 8
QUARTER = 16
CAP = 5
TOKENS = 512
N_PIPE = 8
N_TENSOR = 4
N_EXPERT = 8


def steps_of(rng, shape, shards, low, top_value):
    loudness, own = 1.0, jax.random.fold_in(rng, 6)
    for dim, parts in shards:
        steps = jnp.exp(jax.random.uniform(jax.random.fold_in(own, dim), (parts,), jnp.float32, low / len(shards), top_value / len(shards)))
        loudness = loudness * jnp.repeat(steps, shape[dim] // parts).reshape([-1 if axis == dim else 1 for axis in range(len(shape))])
    return loudness


def different_ones(stream_key, rows, number_of, top, lift):
    sequence = jax.random.permutation(jax.random.fold_in(stream_key, 1), number_of)
    pull = sequence
    for power in range(3):
        pull = pull * pull // number_of
    pull = pull * lift // number_of
    lots = jax.random.randint(jax.random.fold_in(stream_key, 2), (rows, number_of), 0, 4096) + pull
    fixed_rows = jax.random.permutation(jax.random.fold_in(stream_key, 3), rows)[jnp.arange(number_of) % rows]
    lots = jnp.where(jnp.arange(rows)[:, None] == fixed_rows[None, :], 1 << 14, lots)
    priority = lots * number_of + jnp.arange(number_of)
    return lax.top_k(priority.astype(jnp.int32), top)[1].astype(jnp.int32)


def gaussian(key, shape, deviation, most, pieces=(), kind=jnp.bfloat16):
    values = jax.random.normal(key, shape, jnp.float32) * deviation
    if len(pieces) > 0:
        values = steps_of(key, shape, pieces, -0.22, 0.18) * values
    return jnp.clip(values, min=-most, max=most).astype(kind)


def setup_inputs(seed: int = 0) -> dict:
    key_list = jax.random.split(jax.random.key(seed), 9)
    tokens = gaussian(key_list[0], (MICRO, TOKENS, D), 1.0, 6.0, ((1, 8),))
    gains = jnp.clip(1.0 + 0.18 * jax.random.normal(key_list[1], (N_PIPE, D), jnp.float32), 0.1, 1.9)
    route_ids = different_ones(key_list[2], N_PIPE * MICRO * TOKENS, EXPERTS, TOPK, 4096).reshape((N_PIPE, MICRO, TOKENS, TOPK))
    route_weights = jnp.clip(0.2 + 0.8 * jax.random.uniform(key_list[3], (N_PIPE, MICRO, TOKENS, TOPK), jnp.float32) ** steps_of(key_list[3], (N_PIPE, MICRO, TOKENS, TOPK), ((0, 8), (2, 8)), -0.2, 0.2), 0.2, 1.0)
    picks = jax.vmap(lambda own: jax.random.permutation(own, TOK_DEV))(jax.random.split(key_list[4], N_PIPE * MICRO * N_EXPERT)).reshape((N_PIPE, MICRO, N_EXPERT, TOK_DEV)).astype(jnp.int32)
    w_gate = gaussian(key_list[5], (N_PIPE, EXPERTS, D, FF), D ** -0.5, 0.09375, ((0, 8), (1, 8), (3, 4)))
    w_up = gaussian(key_list[6], (N_PIPE, EXPERTS, D, FF), D ** -0.5, 0.09375, ((0, 8), (1, 8), (3, 4)))
    w_down = gaussian(key_list[7], (N_PIPE, EXPERTS, FF, D), FF ** -0.5, 0.15625, ((0, 8), (1, 8), (2, 4)))
    return dict(tokens=tokens, gains=gains, route_ids=route_ids, route_weights=route_weights, picks=picks, w_gate=w_gate, w_up=w_up, w_down=w_down)


epsilon = 1e-06

def find_slots(ordered_ids, capacity):
    onehot = (ordered_ids[..., None] == jnp.arange(EXPERTS, dtype=jnp.int32)).astype(jnp.int32)
    earlier = jnp.cumsum(onehot, axis=-2) - onehot
    slot_index = lax.optimization_barrier(jnp.sum(earlier * onehot, axis=-1))
    return (slot_index, slot_index < capacity)

def expert_ffn(operands):
    row_block, gate_matrix, up_matrix, down_matrix = operands
    gate_val = jnp.dot(row_block, gate_matrix, preferred_element_type=jnp.float32)
    up_val = jnp.dot(row_block, up_matrix, preferred_element_type=jnp.float32)
    hidden = (jax.nn.silu(gate_val) * up_val).astype(jnp.bfloat16)
    shard_width = FF // N_TENSOR
    summed = jnp.zeros((row_block.shape[0], D), jnp.float32)
    for shard_index in range(N_TENSOR):
        lower = shard_index * shard_width
        partial_sum = jnp.dot(hidden[:, lower:lower + shard_width], down_matrix[lower:lower + shard_width], preferred_element_type=jnp.float32)
        rounded = lax.optimization_barrier(partial_sum.astype(jnp.bfloat16))
        summed = summed + rounded.astype(jnp.float32)
    return summed.astype(jnp.bfloat16)

def moe_section(stream, gain_row, section_ids, section_weights, section_picks, gate_all, up_all, down_all):
    groups = N_EXPERT
    offsets = (jnp.arange(groups, dtype=jnp.int32) * TOK_DEV)[:, None]
    ordered = (section_picks + offsets).astype(jnp.int32).reshape(groups, N_TENSOR, QUARTER)
    stream_f = stream.astype(jnp.float32)
    inv_rms = lax.rsqrt(lax.optimization_barrier(jnp.mean(stream_f * stream_f, axis=1, keepdims=True)) + epsilon)
    normed = (stream_f * inv_rms * gain_row[None, :]).astype(jnp.bfloat16)
    ordered_ids = section_ids[ordered].reshape(groups, N_TENSOR, QUARTER * TOPK)
    ordered_weights = section_weights[ordered].reshape(groups, N_TENSOR, QUARTER * TOPK)
    slot_index, kept_mask = find_slots(ordered_ids, CAP)
    route_tokens = jnp.repeat(ordered, TOPK, axis=2)
    group_index = jnp.arange(groups, dtype=jnp.int32)[:, None, None]
    rank_index = jnp.arange(N_TENSOR, dtype=jnp.int32)[None, :, None]
    position = ((ordered_ids * groups + group_index) * N_TENSOR + rank_index) * CAP + slot_index
    filled = EXPERTS * groups * N_TENSOR * CAP
    target = jnp.where(kept_mask, position, filled).astype(jnp.int32)
    source = jnp.full((filled + 1,), TOKENS, jnp.int32).at[target.reshape(-1)].set(route_tokens.reshape(-1))
    padded = jnp.concatenate([normed, jnp.zeros((1, D), jnp.bfloat16)], axis=0)
    row_block = padded[source[:filled]].reshape(EXPERTS, groups * N_TENSOR * CAP, D)
    results = lax.map(expert_ffn, (row_block, gate_all, up_all, down_all))
    flat_results = jnp.concatenate([results.reshape(filled, D), jnp.zeros((1, D), jnp.bfloat16)], axis=0)
    picked = flat_results[target].astype(jnp.float32)
    weighted = picked * (ordered_weights * kept_mask)[..., None]
    update = lax.optimization_barrier(jnp.sum(weighted.reshape(groups, N_TENSOR, QUARTER, TOPK, D), axis=3))
    stream_new = stream_f.at[ordered.reshape(-1)].add(update.reshape(-1, D))
    return stream_new.astype(jnp.bfloat16)

def reference(tokens, gains, route_ids, route_weights, picks, w_gate, w_up, w_down):
    finished = []
    for micro_index in range(MICRO):
        stream = tokens[micro_index]
        column = []
        for section_index in range(N_PIPE):
            stream = moe_section(stream, gains[section_index], route_ids[section_index, micro_index], route_weights[section_index, micro_index], picks[section_index, micro_index], w_gate[section_index], w_up[section_index], w_down[section_index])
            column.append(stream)
        finished.append(jnp.stack(column))
    return jnp.stack(finished, axis=1)
```

```python
import jax
import jax.numpy as jnp
from jax import lax
from jax.sharding import PartitionSpec as P

epsilon = 1e-06
bf16 = jnp.bfloat16
f32 = jnp.float32


def shifted(block, axis, distance):
    size = lax.axis_size(axis)
    return lax.ppermute(block, axis, [(i, (i + distance) % size) for i in range(size)])


def core_swap(block):
    size = lax.axis_size("expert")
    return lax.ppermute(block, "expert", [(i, i ^ 1) for i in range(size)])


def local(tokens, gains, route_ids, route_weights, picks, w_gate, w_up, w_down):
    micro_count, local_tokens, model_width = tokens.shape
    route_count = route_ids.shape[3]
    ranks = lax.axis_size("tensor")
    groups = lax.axis_size("expert")
    sections = lax.axis_size("pipe")
    chips = groups // 2
    quarter = local_tokens // ranks
    capacity = 4 * quarter * route_count // (3 * groups)
    width = model_width // ranks
    per_pair = ranks * capacity
    rows = groups * per_pair
    section = lax.axis_index("pipe")
    rank = lax.axis_index("tensor")
    group = lax.axis_index("expert")
    chip, core = group // 2, group % 2

    shifts = (2, 1, 3)

    def slice_of(value, index, dim):
        return lax.dynamic_slice_in_dim(value, (index % ranks) * width, width, dim)

    def arriving(value, dim):
        return jnp.concatenate([slice_of(value, rank - k + ranks, dim) for k in (0, *shifts)], axis=dim)

    def leaving(value, dim):
        return jnp.concatenate([slice_of(value, rank + k, dim) for k in (0, *shifts)], axis=dim)

    gain_row = arriving(gains, 1)
    in_matrix = arriving(jnp.concatenate([w_gate[0, 0], w_up[0, 0]], axis=1), 0)
    down_matrix = leaving(w_down[0, 0], 1)
    hidden_width = w_gate.shape[3]

    def routing(micro):
        order = picks[0, micro, 0]
        token = jnp.arange(local_tokens, dtype=jnp.int32)
        spot = jnp.arange(local_tokens, dtype=jnp.int32)
        place = jnp.sum(jnp.where(order[None, :] == token[:, None], spot[None, :], 0), axis=1)
        key = (place[:, None] * route_count + jnp.arange(route_count, dtype=jnp.int32)[None, :]).reshape(-1)
        ids = route_ids[0, micro].reshape(-1)
        part = key // (quarter * route_count)
        ahead = (
            (part[:, None] == part[None, :])
            & (ids[:, None] == ids[None, :])
            & (key[None, :] < key[:, None])
        )
        slot = jnp.sum(ahead.astype(jnp.int32), axis=1)
        away = (ids // 2 - chip + chips) % chips
        other = (ids % 2 + core) % 2
        row = ((other * chips + away) * ranks + part) * capacity + slot
        row = jnp.where(slot < capacity, row, rows).reshape(local_tokens, route_count)
        hits = row[:, :, None] == jnp.arange(rows, dtype=jnp.int32)[None, None, :]
        placing = jnp.any(hits, axis=1).astype(bf16)
        mixing = jnp.sum(jnp.where(hits, route_weights[0, micro][:, :, None], 0.0), axis=1)
        high = mixing.astype(bf16)
        low = (mixing - high.astype(f32)).astype(bf16)
        return placing.T, jnp.concatenate([high, low], axis=1)

    tables = [routing(micro) for micro in range(micro_count)]
    placings = jnp.stack([table[0] for table in tables])
    mixings = jnp.stack([table[1] for table in tables])
    own_tokens = lax.dynamic_slice_in_dim(tokens, rank * width, width, 2)

    def to_experts(block):
        block = block.reshape(2, chips, per_pair, width)
        guests = core_swap(block[1])
        paired = jnp.stack([block[0], guests], axis=1)
        moved = {k: shifted(paired[k], "expert", 2 * k) for k in shifts}
        moved[0] = paired[0]
        return jnp.stack([moved[k] for k in range(chips)]).reshape(rows, width)

    def to_home(block):
        paired = block.reshape(chips, 2, per_pair, width)
        moved = {k: shifted(paired[k], "expert", groups - 2 * k) for k in shifts}
        moved[0] = paired[0]
        back = jnp.stack([moved[k] for k in range(chips)], axis=1)
        guests = core_swap(back[1])
        return jnp.concatenate([back[0], guests]).reshape(rows, width)

    def expert_work(own):
        pieces = [own] + [shifted(own, "tensor", k) for k in shifts]
        whole = jnp.concatenate(pieces, axis=1).astype(f32)
        inv_rms = lax.rsqrt(jnp.mean(whole * whole, axis=1, keepdims=True) + epsilon)
        normed = (whole * inv_rms * gain_row).astype(bf16)
        both = jnp.dot(normed, in_matrix, preferred_element_type=f32)
        hidden = (jax.nn.silu(both[:, :hidden_width]) * both[:, hidden_width:]).astype(bf16)
        partial = jnp.dot(hidden, down_matrix, preferred_element_type=f32).astype(bf16)
        total = partial[:, :width].astype(f32)
        for place, k in enumerate(shifts, 1):
            sent = shifted(partial[:, place * width : (place + 1) * width], "tensor", k)
            total = total + sent.astype(f32)
        return total.astype(bf16)

    def tick(arrived, index):
        micro = jnp.clip(index - section, 0, micro_count - 1)
        stream = jnp.where(section == 0, own_tokens[micro], arrived)
        outgoing = jnp.dot(placings[micro], stream, preferred_element_type=f32).astype(bf16)
        returned = to_home(expert_work(to_experts(outgoing)))
        mixing = mixings[micro]
        update = jnp.dot(mixing[:, :rows], returned, preferred_element_type=f32)
        update = update + jnp.dot(mixing[:, rows:], returned, preferred_element_type=f32)
        fresh = (stream.astype(f32) + update).astype(bf16)
        sent = lax.ppermute(fresh, "pipe", [(i, i + 1) for i in range(sections - 1)])
        return sent, fresh

    start = jnp.zeros((local_tokens, width), bf16)
    ticks = jnp.arange(micro_count + sections - 1, dtype=jnp.int32)
    unused, history = lax.scan(tick, start, ticks)
    return lax.dynamic_slice_in_dim(history, section, micro_count)[None]


def solution(mesh):
    return jax.shard_map(
        local,
        mesh=mesh,
        in_specs=(
            P(None, "expert", None),
            P("pipe", None),
            P("pipe", None, "expert", None),
            P("pipe", None, "expert", None),
            P("pipe", None, "expert", None),
            P("pipe", "expert", None, "tensor"),
            P("pipe", "expert", None, "tensor"),
            P("pipe", "expert", "tensor", None),
        ),
        out_specs=P("pipe", None, "expert", "tensor"),
        check_vma=False,
    )
```

```python
import jax
import jax.numpy as jnp
from jax import lax
from jax.sharding import PartitionSpec as P

epsilon = 1e-06
bf16 = jnp.bfloat16
f32 = jnp.float32
i32 = jnp.int32


def shifted(block, axis, distance):
    size = lax.axis_size(axis)
    return lax.ppermute(block, axis, [(i, (i + distance) % size) for i in range(size)])


def core_swap(block):
    size = lax.axis_size("expert")
    return lax.ppermute(block, "expert", [(i, i ^ 1) for i in range(size)])


def onward(block, chips_on):
    sections, groups = lax.axis_size("pipe"), lax.axis_size("expert")
    route = [
        (s * groups + e, ((s + 1) % sections) * groups + (e + 2 * chips_on) % groups)
        for s in range(sections)
        for e in range(groups)
    ]
    return lax.ppermute(block, ("pipe", "expert"), route)


def local(tokens, gains, route_ids, route_weights, picks, w_gate, w_up, w_down):
    micro_count, local_tokens, model_width = tokens.shape
    route_count = route_ids.shape[3]
    ranks = lax.axis_size("tensor")
    groups = lax.axis_size("expert")
    sections = lax.axis_size("pipe")
    chips = groups // 2
    quarter = local_tokens // ranks
    capacity = 4 * quarter * route_count // (3 * groups)
    width = model_width // ranks
    hidden_width = w_gate.shape[3]
    per_pair = ranks * capacity
    per_chip = 2 * per_pair
    rows = chips * per_chip
    section = lax.axis_index("pipe")
    rank = lax.axis_index("tensor")
    group = lax.axis_index("expert")
    chip, core = group // 2, group % 2
    chip_shifts = (2, 1, 3)
    rank_shifts = (2, 1, 3)
    pieces = (0, *rank_shifts)

    def slice_at(value, index, dim):
        return lax.dynamic_slice_in_dim(value, ((index + ranks) % ranks) * width, width, dim)

    def by_core(mine, guest):
        first = jnp.where(core == 0, mine, guest)
        second = jnp.where(core == 0, guest, mine)
        return jnp.concatenate([first, second], axis=1)

    numbers = jnp.concatenate([route_ids[0], picks[0, :, 0, :, None]], axis=2)
    numbers = by_core(numbers, core_swap(numbers))
    weights = by_core(route_weights[0], core_swap(route_weights[0]))
    own_slice = lax.dynamic_slice_in_dim(tokens, rank * width, width, 2)
    entering = by_core(own_slice, core_swap(own_slice))

    def hits_of(known):
        order = known[:, route_count].reshape(2, local_tokens)
        token = jnp.arange(local_tokens, dtype=i32)
        place = jnp.sum(jnp.where(order[:, None, :] == token[None, :, None], token[None, None, :], 0), axis=2)
        key = place[:, :, None] * route_count + jnp.arange(route_count, dtype=i32)[None, None, :]
        key = key.reshape(2, local_tokens * route_count)
        ids = known[:, :route_count].reshape(2, local_tokens * route_count)
        part = key // (quarter * route_count)
        line = ids * ranks + part
        ahead = (line[:, :, None] == line[:, None, :]) & (key[:, None, :] < key[:, :, None])
        slot = jnp.sum(ahead.astype(i32), axis=2)
        away = (ids // 2 - chip + chips) % chips
        home = jnp.arange(2, dtype=i32)[:, None]
        row = away * per_chip + home * per_pair + part * capacity + slot
        row = jnp.where((slot < capacity) & (ids % 2 == core), row, rows)
        row = row.reshape(2 * local_tokens, route_count)
        return row[:, :, None] == jnp.arange(rows, dtype=i32)[None, None, :]

    def placing_of(known):
        return jnp.any(hits_of(known), axis=1).astype(bf16).T

    def mixing_of(known, weight):
        mixing = jnp.sum(jnp.where(hits_of(known), weight[:, :, None], 0.0), axis=1)
        high = mixing.astype(bf16)
        low = (mixing - high.astype(f32)).astype(bf16)
        return jnp.concatenate([high, low], axis=1)

    def dispatched(placing, stream):
        outgoing = jnp.dot(placing, stream, preferred_element_type=f32).astype(bf16)
        return outgoing.reshape(chips, per_chip, width)

    outgoing = dispatched(placing_of(numbers[0]), entering[0])
    moved = {k: shifted(outgoing[k], "expert", 2 * k) for k in chip_shifts}
    moved[0] = outgoing[0]
    first_rows = jnp.concatenate([moved[k] for k in range(chips)])

    next_numbers = shifted(numbers, "pipe", sections - 1)
    placings = jnp.stack([placing_of(next_numbers[m]) for m in range(micro_count)])
    mixings = jnp.stack([mixing_of(numbers[m], weights[m]) for m in range(micro_count)])

    down_parts = [slice_at(w_down[0, 0], rank, 1)]
    down_parts += [shifted(slice_at(w_down[0, 0], rank + k, 1), "tensor", k) for k in rank_shifts]
    gain_parts = [slice_at(gains, rank - k, 1) for k in pieces]
    in_parts = [
        jnp.concatenate([slice_at(w_gate[0, 0], rank - k, 0), slice_at(w_up[0, 0], rank - k, 0)], axis=1)
        for k in pieces
    ]

    def expert_work(own, gain_parts, in_parts, down_parts):
        slices = [own] + [shifted(own, "tensor", k) for k in rank_shifts]
        squares, both = 0.0, 0.0
        for piece, gain, matrix in zip(slices, gain_parts, in_parts):
            wide = piece.astype(f32)
            squares = squares + jnp.sum(wide * wide, axis=1, keepdims=True)
            both = both + jnp.dot((wide * gain).astype(bf16), matrix, preferred_element_type=f32)
        both = both * lax.rsqrt(squares / model_width + epsilon)
        hidden = (jax.nn.silu(both[:, :hidden_width]) * both[:, hidden_width:]).astype(bf16)
        hiddens = [hidden] + [shifted(hidden, "tensor", k) for k in rank_shifts]
        total = 0.0
        for part, matrix in zip(hiddens, down_parts):
            total = total + jnp.dot(part, matrix, preferred_element_type=f32)
        return total.astype(bf16)

    def to_home(block):
        block = block.reshape(chips, per_chip, width)
        back = {k: shifted(block[k], "expert", groups - 2 * k) for k in chip_shifts}
        back[0] = block[0]
        return jnp.concatenate([back[k] for k in range(chips)])

    def combined(stream, returned, mixing):
        update = jnp.dot(mixing[:, :rows], returned, preferred_element_type=f32)
        update = update + jnp.dot(mixing[:, rows:], returned, preferred_element_type=f32)
        return (stream.astype(f32) + (update + core_swap(update))).astype(bf16)

    def kept(collected, fresh, spot):
        own = lax.dynamic_slice_in_dim(fresh, core * local_tokens, local_tokens)
        return lax.dynamic_update_slice_in_dim(collected, own[None], spot, 0)

    returned = to_home(expert_work(first_rows, gain_parts, in_parts, down_parts))
    fresh = combined(entering[0], returned, mixings[0])
    collected = jnp.zeros((micro_count + 1, local_tokens, width), bf16)
    collected = kept(collected, fresh, 0)
    fresh = jnp.where(section == sections - 1, entering[1], fresh)

    def tick(index, carry):
        fresh, collected = carry
        unit = index - section
        leaving = jnp.where(section == sections - 1, 1, jnp.clip(unit - 1, 0, micro_count - 1))
        outgoing = dispatched(placings[leaving], fresh)
        moved = {k: onward(outgoing[k], k) for k in (*chip_shifts, 0)}
        arrived = jnp.concatenate([moved[k] for k in range(chips)])
        stream = shifted(fresh, "pipe", 1)
        returned = to_home(expert_work(arrived, gain_parts, in_parts, down_parts))
        fresh = combined(stream, returned, mixings[jnp.clip(unit, 0, micro_count - 1)])
        return fresh, kept(collected, fresh, jnp.clip(unit, 0, micro_count))

    fresh, collected = lax.fori_loop(1, micro_count + sections - 1, tick, (fresh, collected))
    return collected[None, :micro_count]


def solution(mesh):
    return jax.shard_map(
        local,
        mesh=mesh,
        in_specs=(
            P(None, "expert", None),
            P("pipe", None),
            P("pipe", None, "expert", None),
            P("pipe", None, "expert", None),
            P("pipe", None, "expert", None),
            P("pipe", "expert", None, "tensor"),
            P("pipe", "expert", None, "tensor"),
            P("pipe", "expert", "tensor", None),
        ),
        out_specs=P("pipe", None, "expert", "tensor"),
        check_vma=False,
    )
```

```python
import functools

import jax
import jax.numpy as jnp
from jax import lax
from jax.experimental import pallas as pl
from jax.experimental.pallas import tpu as pltpu
from jax.sharding import PartitionSpec as P

epsilon = 1e-06
bf16 = jnp.bfloat16
f32 = jnp.float32
i32 = jnp.int32
SMEM = pl.BlockSpec(memory_space=pltpu.SMEM)
VMEM = pl.BlockSpec(memory_space=pltpu.VMEM)
HBM = pl.BlockSpec(memory_space=pltpu.HBM)
CHIP_SHIFTS = (2, 1, 3)
RANK_SHIFTS = (2, 1, 3)


def kernel_call(body, name, in_specs, out_shapes, mib, scratch=(), flops=0, moved=0):
    return pl.pallas_call(
        body,
        name=name,
        in_specs=in_specs,
        out_specs=jax.tree.map(lambda _: VMEM, out_shapes),
        out_shape=out_shapes,
        scratch_shapes=list(scratch),
        compiler_params=pltpu.CompilerParams(vmem_limit_bytes=mib << 20),
        cost_estimate=pl.CostEstimate(flops=flops, bytes_accessed=moved, transcendentals=0),
    )


def shifted(block, axis, distance):
    size = lax.axis_size(axis)
    return lax.ppermute(block, axis, [(i, (i + distance) % size) for i in range(size)])


def core_swap(block):
    size = lax.axis_size("expert")
    return lax.ppermute(block, "expert", [(i, i ^ 1) for i in range(size)])


def onward(block, chips_on):
    sections, groups = lax.axis_size("pipe"), lax.axis_size("expert")
    route = [
        (s * groups + e, ((s + 1) % sections) * groups + (e + 2 * chips_on) % groups)
        for s in range(sections)
        for e in range(groups)
    ]
    return lax.ppermute(block, ("pipe", "expert"), route)


def tables_kernel(sizes, where, info, place, high, low):
    chips, ranks, quarter, capacity = sizes
    tokens = info.shape[3]
    rows = place.shape[2]
    per_pair = ranks * capacity
    chip, core = where[0].astype(f32), where[1].astype(f32)
    across = lax.broadcasted_iota(i32, (tokens, tokens), 1)
    down = lax.broadcasted_iota(i32, (tokens, tokens), 0)
    across_f, down_f = across.astype(f32), down.astype(f32)
    spots = lax.broadcasted_iota(i32, (tokens, rows), 1).astype(f32)

    def column(row):
        return jnp.sum(jnp.where(across == down, row, 0.0), axis=1, keepdims=True)

    for micro in range(info.shape[0]):
        for home in range(2):
            known = info[micro, home]
            id_rows = [known[k : k + 1] for k in range(2)]
            order = known[2:3]
            place_col = jnp.sum(jnp.where(order == down_f, across_f, 0.0), axis=1, keepdims=True)
            place_row = jnp.sum(jnp.where(column(order) == across_f, down_f, 0.0), axis=0, keepdims=True)
            part_col = jnp.floor(place_col * (1.0 / quarter))
            part_row = jnp.floor(place_row * (1.0 / quarter))
            ahead = (part_col == part_row) & (place_row < place_col)
            span = slice(home * tokens, (home + 1) * tokens)
            hot = jnp.zeros((tokens, rows), f32)
            mixed = jnp.zeros((tokens, rows), f32)
            for k in range(2):
                ids = column(id_rows[k])
                same = jnp.where(id_rows[0] == ids, 1.0, 0.0) + jnp.where(id_rows[1] == ids, 1.0, 0.0)
                slot = jnp.sum(jnp.where(ahead, same, 0.0), axis=1, keepdims=True)
                its_chip = jnp.floor(ids * 0.5)
                away = its_chip - chip
                away = jnp.where(away < 0.0, away + chips, away)
                row = away * (2 * per_pair) + home * per_pair + part_col * capacity + slot
                row = jnp.where((slot < capacity) & (ids - 2.0 * its_chip == core), row, -1.0)
                hit = row == spots
                hot = jnp.where(hit, 1.0, hot)
                mixed = jnp.where(hit, column(known[3 + k : 4 + k]), mixed)
            top = mixed.astype(bf16)
            place[micro, span] = hot.astype(bf16)
            high[micro, span] = top
            low[micro, span] = (mixed - top.astype(f32)).astype(bf16)


def dispatch_kernel(which, place, stream, *outs):
    rows = lax.dot_general(
        place[which[0]], stream[...], (((0,), (0,)), ((), ())), preferred_element_type=f32
    )
    count = outs[0].shape[0]
    for k, out in enumerate(outs):
        out[...] = rows[k * count : (k + 1) * count].astype(bf16)


def combine_kernel(which, high, low, *refs):
    *blocks, out = refs
    rows = jnp.concatenate([block[...].astype(f32) for block in blocks]).astype(bf16)
    update = jnp.dot(high[which[0]], rows, preferred_element_type=f32)
    out[...] = update + jnp.dot(low[which[0]], rows, preferred_element_type=f32)


def gate_up_kernel(shifts, last, model_width, rank, gains, w_gate, w_up, *refs):
    count = len(shifts)
    slices = refs[:count]
    refs = refs[count:]
    if last:
        gate_in, up_in, squares_in, hidden, gate_buf, up_buf, sems = refs
    else:
        gate_out, up_out, squares_out, gate_buf, up_buf, sems = refs
    width = slices[0].shape[1]
    ranks = w_gate.shape[0] // width
    copies = []
    for i, k in enumerate(shifts):
        start = lax.rem(rank[0] + (ranks - k), ranks) * width
        pair = [
            pltpu.make_async_copy(src.at[pl.ds(start, width)], buf.at[i], sems.at[i, j])
            for j, (src, buf) in enumerate(((w_gate, gate_buf), (w_up, up_buf)))
        ]
        for copy in pair:
            copy.start()
        copies.append(pair)
    if last:
        gate, up, squares = gate_in[...], up_in[...], squares_in[:, :1]
    else:
        gate, up, squares = 0.0, 0.0, 0.0
    for i, k in enumerate(shifts):
        wide = slices[i][...].astype(f32)
        squares = squares + jnp.sum(wide * wide, axis=1, keepdims=True)
        scaled = (wide * gains[k : k + 1]).astype(bf16)
        copies[i][0].wait()
        gate = gate + jnp.dot(scaled, gate_buf[i], preferred_element_type=f32)
        copies[i][1].wait()
        up = up + jnp.dot(scaled, up_buf[i], preferred_element_type=f32)
    if last:
        inv_rms = lax.rsqrt(squares * (1.0 / model_width) + epsilon)
        gate = gate * inv_rms
        hidden[...] = (gate / (1.0 + jnp.exp(-gate)) * (up * inv_rms)).astype(bf16)
    else:
        gate_out[...] = gate
        up_out[...] = up
        squares_out[...] = jnp.broadcast_to(squares, squares_out.shape)


def down_kernel(last, count, *refs):
    parts, matrices, refs = refs[:count], refs[count : 2 * count], refs[2 * count :]
    if last:
        before, *outs, buf, sems = refs
    else:
        out, buf, sems = refs
    copies = [pltpu.make_async_copy(matrices[i], buf.at[i], sems.at[i]) for i in range(count)]
    for copy in copies:
        copy.start()
    total = before[...] if last else 0.0
    for i in range(count):
        copies[i].wait()
        total = total + jnp.dot(parts[i][...], buf[i], preferred_element_type=f32)
    if last:
        size = outs[0].shape[0]
        for k, piece in enumerate(outs):
            piece[...] = total[k * size : (k + 1) * size].astype(bf16)
    else:
        out[...] = total


def local(tokens, gains, route_ids, route_weights, picks, w_gate, w_up, w_down):
    micro_count, local_tokens, model_width = tokens.shape
    route_count = route_ids.shape[3]
    ranks = lax.axis_size("tensor")
    groups = lax.axis_size("expert")
    sections = lax.axis_size("pipe")
    chips = groups // 2
    quarter = local_tokens // ranks
    capacity = 4 * quarter * route_count // (3 * groups)
    width = model_width // ranks
    hidden_width = w_gate.shape[3]
    per_chip = 2 * ranks * capacity
    rows = chips * per_chip
    section = lax.axis_index("pipe")
    rank = lax.axis_index("tensor")
    group = lax.axis_index("expert")
    chip, core = group // 2, group % 2
    gate_matrix, up_matrix, down_matrix = w_gate[0, 0], w_up[0, 0], w_down[0, 0]

    def slice_at(value, index, dim):
        return lax.dynamic_slice_in_dim(value, ((index + ranks) % ranks) * width, width, dim)

    def by_core(mine, guest, dim):
        first = jnp.where(core == 0, mine, guest)
        second = jnp.where(core == 0, guest, mine)
        return jnp.concatenate([first, second], axis=dim)

    def shape(*dims, kind=bf16):
        return jax.ShapeDtypeStruct(dims, kind)

    info = jnp.concatenate(
        [route_ids[0].transpose(0, 2, 1).astype(f32), picks[0].astype(f32), route_weights[0].transpose(0, 2, 1)],
        axis=1,
    )[:, None]
    info = by_core(info, core_swap(info), 1)
    where = jnp.stack([chip, core]).astype(i32)
    table = shape(micro_count, 2 * local_tokens, rows)
    tables = kernel_call(
        functools.partial(tables_kernel, (chips, ranks, quarter, capacity)),
        "tables",
        (SMEM, VMEM),
        (table, table, table),
        8,
    )
    first_place, high, low = tables(where, info)

    own_slice = lax.dynamic_slice_in_dim(tokens, rank * width, width, 2)
    entering = by_core(own_slice, core_swap(own_slice), 1)

    dispatch = kernel_call(
        dispatch_kernel, "dispatch", (SMEM, VMEM, VMEM), (shape(per_chip, width),) * chips, 8, flops=10**9
    )
    combine = kernel_call(
        combine_kernel,
        "combine",
        (SMEM, VMEM, VMEM) + (VMEM,) * chips,
        shape(2 * local_tokens, width, kind=f32),
        8,
        flops=10**9,
    )
    half = (shape(rows, hidden_width, kind=f32),) * 2 + (shape(rows, 128, kind=f32),)
    buffers = [pltpu.VMEM((2, width, hidden_width), bf16)] * 2 + [pltpu.SemaphoreType.DMA((2, 2))]
    early, late = (0, 1), (3, 2)
    gate_up = [
        kernel_call(
            functools.partial(gate_up_kernel, shifts, last, model_width),
            name,
            (SMEM, VMEM, HBM, HBM, VMEM, VMEM) + (VMEM,) * (3 * last),
            shape(rows, hidden_width) if last else half,
            16,
            buffers,
            flops=2 * 10**9,
        )
        for name, shifts, last in (("gate_up_a", early, False), ("gate_up_b", late, True))
    ]
    down_buffers = [pltpu.VMEM((2, hidden_width, width), bf16), pltpu.SemaphoreType.DMA((2,))]
    down = [
        kernel_call(
            functools.partial(down_kernel, last, 2),
            name,
            (VMEM, VMEM, HBM, HBM) + (VMEM,) * last,
            (shape(per_chip, width),) * chips if last else shape(rows, width, kind=f32),
            10,
            down_buffers,
            flops=10**9,
        )
        for name, last in (("down_a", False), ("down_b", True))
    ]

    rank_word = rank.reshape(1).astype(i32)
    gain_parts = jnp.concatenate([slice_at(gains, rank - k, 1) for k in range(ranks)])

    def expert_work(blocks, down_parts, also):
        own = jnp.concatenate(blocks)
        slices = {k: shifted(own, "tensor", k) for k in RANK_SHIFTS}
        slices[0] = own
        weights = (rank_word, gain_parts, gate_matrix, up_matrix)
        partial = gate_up[0](*weights, *(slices[k] for k in early))
        hidden = gate_up[1](*weights, *(slices[k] for k in late), *partial)
        hidden, also = lax.optimization_barrier((hidden, also))
        hiddens = {k: shifted(hidden, "tensor", k) for k in RANK_SHIFTS}
        hiddens[0] = hidden
        total = down[0](*(hiddens[k] for k in early), *(down_parts[k] for k in early))
        return down[1](*(hiddens[k] for k in late), *(down_parts[k] for k in late), total), also

    def to_home(blocks):
        back = {k: shifted(blocks[k], "expert", groups - 2 * k) for k in CHIP_SHIFTS}
        back[0] = blocks[0]
        return [back[k] for k in range(chips)]

    def combined(stream, blocks, which):
        update = combine(which.reshape(1), high, low, *blocks)
        return (stream.astype(f32) + (update + core_swap(update))).astype(bf16)

    def kept(collected, fresh, spot):
        own = lax.dynamic_slice_in_dim(fresh, core * local_tokens, local_tokens)
        return lax.dynamic_update_slice_in_dim(collected, own[None], spot, 0)

    outgoing = dispatch(jnp.zeros(1, i32), first_place, entering[0])
    moved = {k: shifted(outgoing[k], "expert", 2 * k) for k in CHIP_SHIFTS}
    moved[0] = outgoing[0]

    down_parts = {k: shifted(slice_at(down_matrix, rank + k, 1), "tensor", k) for k in RANK_SHIFTS}
    down_parts[0] = slice_at(down_matrix, rank, 1)
    next_info = shifted(info, "pipe", sections - 1)
    place = tables(where, next_info)[0]

    blocks, stream = expert_work([moved[k] for k in range(chips)], down_parts, entering[0])
    fresh = combined(stream, to_home(blocks), jnp.zeros((), i32))
    collected = kept(jnp.zeros((micro_count + 1, local_tokens, width), bf16), fresh, 0)
    fresh = jnp.where(section == sections - 1, entering[1], fresh)

    def tick(index, carry):
        fresh, collected = carry
        unit = index - section
        leaving = jnp.where(section == sections - 1, 1, jnp.clip(unit - 1, 0, micro_count - 1))
        outgoing = dispatch(leaving.reshape(1), place, fresh)
        moved = {k: onward(outgoing[k], k) for k in (*CHIP_SHIFTS, 0)}
        stream = shifted(fresh, "pipe", 1)
        blocks, stream = expert_work([moved[k] for k in range(chips)], down_parts, stream)
        fresh = combined(stream, to_home(blocks), jnp.clip(unit, 0, micro_count - 1))
        return fresh, kept(collected, fresh, jnp.clip(unit, 0, micro_count))

    fresh, collected = lax.fori_loop(1, micro_count + sections - 1, tick, (fresh, collected))
    return collected[None, :micro_count]


def solution(mesh):
    return jax.shard_map(
        local,
        mesh=mesh,
        in_specs=(
            P(None, "expert", None),
            P("pipe", None),
            P("pipe", None, "expert", None),
            P("pipe", None, "expert", None),
            P("pipe", None, "expert", None),
            P("pipe", "expert", None, "tensor"),
            P("pipe", "expert", None, "tensor"),
            P("pipe", "expert", "tensor", None),
        ),
        out_specs=P("pipe", None, "expert", "tensor"),
        check_vma=False,
    )
```

```python
import functools

import jax
import jax.numpy as jnp
from jax import lax
from jax.experimental import pallas as pl
from jax.experimental.pallas import tpu as pltpu
from jax.sharding import PartitionSpec as P

epsilon = 1e-06
bf16 = jnp.bfloat16
f32 = jnp.float32
i32 = jnp.int32
SMEM = pl.BlockSpec(memory_space=pltpu.SMEM)
VMEM = pl.BlockSpec(memory_space=pltpu.VMEM)
HBM = pl.BlockSpec(memory_space=pltpu.HBM)
CHIP_SHIFTS = (2, 1, 3)
RANK_SHIFTS = (2, 1, 3)


def kernel_call(body, in_specs, out_shapes, mib, scratch=(), flops=0, moved=0):
    return pl.pallas_call(
        body,
        in_specs=in_specs,
        out_specs=jax.tree.map(lambda _: VMEM, out_shapes),
        out_shape=out_shapes,
        scratch_shapes=list(scratch),
        compiler_params=pltpu.CompilerParams(vmem_limit_bytes=mib << 20),
        cost_estimate=pl.CostEstimate(flops=flops, bytes_accessed=moved, transcendentals=0),
    )


def in_hbm(value):
    return pltpu.with_memory_space_constraint(value, pltpu.HBM)


def shifted(block, axis, distance):
    size = lax.axis_size(axis)
    return lax.ppermute(block, axis, [(i, (i + distance) % size) for i in range(size)])


def core_swap(block):
    size = lax.axis_size("expert")
    return lax.ppermute(block, "expert", [(i, i ^ 1) for i in range(size)])


def onward(block, chips_on):
    sections, groups = lax.axis_size("pipe"), lax.axis_size("expert")
    route = [
        (s * groups + e, ((s + 1) % sections) * groups + (e + 2 * chips_on) % groups)
        for s in range(sections)
        for e in range(groups)
    ]
    return lax.ppermute(block, ("pipe", "expert"), route)


def tables_kernel(sizes, where, info, place, high, low):
    chips, ranks, quarter, capacity = sizes
    tokens = info.shape[3]
    rows = place.shape[2]
    per_pair = ranks * capacity
    chip, core = where[0].astype(f32), where[1].astype(f32)
    across = lax.broadcasted_iota(i32, (tokens, tokens), 1)
    down = lax.broadcasted_iota(i32, (tokens, tokens), 0)
    across_f, down_f = across.astype(f32), down.astype(f32)
    spots = lax.broadcasted_iota(i32, (tokens, rows), 1).astype(f32)

    def column(row):
        return jnp.sum(jnp.where(across == down, row, 0.0), axis=1, keepdims=True)

    for micro in range(info.shape[0]):
        for home in range(2):
            known = info[micro, home]
            id_rows = [known[k : k + 1] for k in range(2)]
            order = known[2:3]
            place_col = jnp.sum(jnp.where(order == down_f, across_f, 0.0), axis=1, keepdims=True)
            place_row = jnp.sum(jnp.where(column(order) == across_f, down_f, 0.0), axis=0, keepdims=True)
            part_col = jnp.floor(place_col * (1.0 / quarter))
            part_row = jnp.floor(place_row * (1.0 / quarter))
            ahead = (part_col == part_row) & (place_row < place_col)
            span = slice(home * tokens, (home + 1) * tokens)
            hot = jnp.zeros((tokens, rows), f32)
            mixed = jnp.zeros((tokens, rows), f32)
            for k in range(2):
                ids = column(id_rows[k])
                same = jnp.where(id_rows[0] == ids, 1.0, 0.0) + jnp.where(id_rows[1] == ids, 1.0, 0.0)
                slot = jnp.sum(jnp.where(ahead, same, 0.0), axis=1, keepdims=True)
                its_chip = jnp.floor(ids * 0.5)
                away = its_chip - chip
                away = jnp.where(away < 0.0, away + chips, away)
                row = away * (2 * per_pair) + home * per_pair + part_col * capacity + slot
                row = jnp.where((slot < capacity) & (ids - 2.0 * its_chip == core), row, -1.0)
                hit = row == spots
                hot = jnp.where(hit, 1.0, hot)
                mixed = jnp.where(hit, column(known[3 + k : 4 + k]), mixed)
            top = mixed.astype(bf16)
            place[micro, span] = hot.astype(bf16)
            high[micro, span] = top
            low[micro, span] = (mixed - top.astype(f32)).astype(bf16)


def dispatch_kernel(which, place, stream, *outs):
    rows = lax.dot_general(
        place[which[0]], stream[...], (((0,), (0,)), ((), ())), preferred_element_type=f32
    )
    count = outs[0].shape[0]
    for k, out in enumerate(outs):
        out[...] = rows[k * count : (k + 1) * count].astype(bf16)


def combine_kernel(which, high, low, *refs):
    *blocks, out = refs
    rows = jnp.concatenate([block[...].astype(f32) for block in blocks]).astype(bf16)
    update = jnp.dot(high[which[0]], rows, preferred_element_type=f32)
    out[...] = update + jnp.dot(low[which[0]], rows, preferred_element_type=f32)


def gate_up_first(early, late, rank, gains, w_gate, w_up, *refs):
    count, downs = len(early), len(early) + len(late)
    w_down, refs = refs[:downs], refs[downs:]
    slices, refs = refs[:count], refs[count:]
    gate_out, up_out, squares_out, gate_late, up_late, down_out, gate_buf, up_buf, sems, late_sems, down_sems = refs
    width = slices[0].shape[1]
    ranks = w_gate.shape[0] // width

    def pair(k, i, gate_to, up_to, sems):
        start = lax.rem(rank[0] + (ranks - k), ranks) * width
        return [
            pltpu.make_async_copy(w_gate.at[pl.ds(start, width)], gate_to.at[i], sems.at[i, 0]),
            pltpu.make_async_copy(w_up.at[pl.ds(start, width)], up_to.at[i], sems.at[i, 1]),
        ]

    now = [pair(k, i, gate_buf, up_buf, sems) for i, k in enumerate(early)]
    later = [copy for i, k in enumerate(late) for copy in pair(k, i, gate_late, up_late, late_sems)]
    later += [pltpu.make_async_copy(w_down[i], down_out.at[i], down_sems.at[i]) for i in range(downs)]
    for copy in [*now[0], *now[1], *later]:
        copy.start()
    gate, up, squares = 0.0, 0.0, 0.0
    for i, k in enumerate(early):
        wide = slices[i][...].astype(f32)
        squares = squares + jnp.sum(wide * wide, axis=1, keepdims=True)
        scaled = (wide * gains[k : k + 1]).astype(bf16)
        now[i][0].wait()
        gate = gate + jnp.dot(scaled, gate_buf[i], preferred_element_type=f32)
        now[i][1].wait()
        up = up + jnp.dot(scaled, up_buf[i], preferred_element_type=f32)
    gate_out[...] = gate
    up_out[...] = up
    squares_out[...] = jnp.broadcast_to(squares, squares_out.shape)
    for copy in later:
        copy.wait()


def gate_up_last(late, model_width, gains, gate_late, up_late, gate_in, up_in, squares_in, *refs):
    *slices, hidden = refs
    gate, up, squares = gate_in[...], up_in[...], squares_in[:, :1]
    for i, k in enumerate(late):
        wide = slices[i][...].astype(f32)
        squares = squares + jnp.sum(wide * wide, axis=1, keepdims=True)
        scaled = (wide * gains[k : k + 1]).astype(bf16)
        gate = gate + jnp.dot(scaled, gate_late[i], preferred_element_type=f32)
        up = up + jnp.dot(scaled, up_late[i], preferred_element_type=f32)
    inv_rms = lax.rsqrt(squares * (1.0 / model_width) + epsilon)
    gate = gate * inv_rms
    hidden[...] = (gate / (1.0 + jnp.exp(-gate)) * (up * inv_rms)).astype(bf16)


def down_first(matrices, own, guest, out):
    out[...] = jnp.dot(own[...], matrices[0], preferred_element_type=f32) + jnp.dot(
        guest[...], matrices[1], preferred_element_type=f32
    )


def down_last(matrices, before, one, other, *outs):
    total = before[...] + jnp.dot(one[...], matrices[2], preferred_element_type=f32)
    total = total + jnp.dot(other[...], matrices[3], preferred_element_type=f32)
    size = outs[0].shape[0]
    for k, piece in enumerate(outs):
        piece[...] = total[k * size : (k + 1) * size].astype(bf16)


def local(tokens, gains, route_ids, route_weights, picks, w_gate, w_up, w_down):
    micro_count, local_tokens, model_width = tokens.shape
    route_count = route_ids.shape[3]
    ranks = lax.axis_size("tensor")
    groups = lax.axis_size("expert")
    sections = lax.axis_size("pipe")
    chips = groups // 2
    quarter = local_tokens // ranks
    capacity = 4 * quarter * route_count // (3 * groups)
    width = model_width // ranks
    hidden_width = w_gate.shape[3]
    per_chip = 2 * ranks * capacity
    rows = chips * per_chip
    section = lax.axis_index("pipe")
    rank = lax.axis_index("tensor")
    group = lax.axis_index("expert")
    chip, core = group // 2, group % 2
    gate_matrix, up_matrix, down_matrix = w_gate[0, 0], w_up[0, 0], w_down[0, 0]

    def slice_at(value, index, dim):
        return lax.dynamic_slice_in_dim(value, ((index + ranks) % ranks) * width, width, dim)

    def by_core(mine, guest, dim):
        first = jnp.where(core == 0, mine, guest)
        second = jnp.where(core == 0, guest, mine)
        return jnp.concatenate([first, second], axis=dim)

    def shape(*dims, kind=bf16):
        return pltpu.VMEM(dims, kind)

    down_parts = {k: shifted(slice_at(down_matrix, rank + k, 1), "tensor", k) for k in RANK_SHIFTS}
    down_parts[0] = slice_at(down_matrix, rank, 1)

    info = jnp.concatenate(
        [route_ids[0].transpose(0, 2, 1).astype(f32), picks[0].astype(f32), route_weights[0].transpose(0, 2, 1)],
        axis=1,
    )[:, None]
    info = by_core(info, core_swap(info), 1)
    where = jnp.stack([chip, core]).astype(i32)
    table = shape(micro_count, 2 * local_tokens, rows)
    tables = kernel_call(
        functools.partial(tables_kernel, (chips, ranks, quarter, capacity)), (SMEM, VMEM), (table, table, table), 8
    )
    first_place, high, low = tables(where, info)

    own_slice = lax.dynamic_slice_in_dim(tokens, rank * width, width, 2)
    entering = by_core(own_slice, core_swap(own_slice), 1)

    dispatch = kernel_call(dispatch_kernel, (SMEM, VMEM, VMEM), (shape(per_chip, width),) * chips, 8, flops=10**9)
    combine = kernel_call(
        combine_kernel, (SMEM, VMEM, VMEM) + (VMEM,) * chips, shape(2 * local_tokens, width, kind=f32), 8, flops=10**9
    )
    early, late = (0, 1), (3, 2)
    gate_up_a = kernel_call(
        functools.partial(gate_up_first, early, late),
        (SMEM, VMEM, HBM, HBM) + (HBM,) * ranks + (VMEM,) * 2,
        (shape(rows, hidden_width, kind=f32),) * 2
        + (shape(rows, 128, kind=f32),)
        + (shape(2, width, hidden_width),) * 2
        + (shape(ranks, hidden_width, width),),
        24,
        [pltpu.VMEM((2, width, hidden_width), bf16)] * 2
        + [pltpu.SemaphoreType.DMA((2, 2)), pltpu.SemaphoreType.DMA((2, 2)), pltpu.SemaphoreType.DMA((ranks,))],
        flops=3 * 10**9,
    )
    gate_up_b = kernel_call(
        functools.partial(gate_up_last, late, model_width), (VMEM,) * 8, shape(rows, hidden_width), 16, flops=10**9
    )
    down_a = kernel_call(down_first, (VMEM,) * 3, shape(rows, width, kind=f32), 16, flops=5 * 10**8)
    down_b = kernel_call(down_last, (VMEM,) * 4, (shape(per_chip, width),) * chips, 16, flops=5 * 10**8)

    rank_word = rank.reshape(1).astype(i32)
    gain_parts = jnp.concatenate([slice_at(gains, rank - k, 1) for k in range(ranks)])

    def expert_work(blocks, down_parts, also):
        own = jnp.concatenate(blocks)
        slices = {k: shifted(own, "tensor", k) for k in RANK_SHIFTS}
        slices[0] = own
        weights = [in_hbm(value) for value in (gate_matrix, up_matrix, *(down_parts[k] for k in (*early, *late)))]
        gate, up, squares, gate_late, up_late, matrices = gate_up_a(
            rank_word, gain_parts, *weights, *(slices[k] for k in early)
        )
        hidden = gate_up_b(gain_parts, gate_late, up_late, gate, up, squares, *(slices[k] for k in late))
        hidden, also = lax.optimization_barrier((hidden, also))
        hiddens = {k: shifted(hidden, "tensor", k) for k in RANK_SHIFTS}
        hiddens[0] = hidden
        total = down_a(matrices, *(hiddens[k] for k in early))
        return down_b(matrices, total, *(hiddens[k] for k in late)), also

    def to_home(blocks):
        back = {k: shifted(blocks[k], "expert", groups - 2 * k) for k in CHIP_SHIFTS}
        back[0] = blocks[0]
        return [back[k] for k in range(chips)]

    def combined(stream, blocks, which):
        update = combine(which.reshape(1), high, low, *blocks)
        return (stream.astype(f32) + (update + core_swap(update))).astype(bf16)

    def kept(collected, fresh, spot):
        own = lax.dynamic_slice_in_dim(fresh, core * local_tokens, local_tokens)[None]
        held = lax.dynamic_slice_in_dim(collected, jnp.minimum(spot, micro_count - 1), 1)
        own = jnp.where(spot < micro_count, own, held)
        return lax.dynamic_update_slice_in_dim(collected, own, jnp.minimum(spot, micro_count - 1), 0)

    outgoing = dispatch(jnp.zeros(1, i32), first_place, entering[0])
    moved = {k: shifted(outgoing[k], "expert", 2 * k) for k in CHIP_SHIFTS}
    moved[0] = outgoing[0]

    next_info = shifted(info, "pipe", sections - 1)
    place = tables(where, next_info)[0]

    blocks, stream = expert_work([moved[k] for k in range(chips)], down_parts, entering[0])
    fresh = combined(stream, to_home(blocks), jnp.zeros((), i32))
    collected = kept(jnp.zeros((micro_count, local_tokens, width), bf16), fresh, 0)
    fresh = jnp.where(section == sections - 1, entering[1], fresh)

    def tick(index, carry):
        fresh, collected = carry
        unit = index - section
        leaving = jnp.where(section == sections - 1, 1, jnp.clip(unit - 1, 0, micro_count - 1))
        outgoing = dispatch(leaving.reshape(1), place, fresh)
        moved = {k: onward(outgoing[k], k) for k in (*CHIP_SHIFTS, 0)}
        stream = shifted(fresh, "pipe", 1)
        blocks, stream = expert_work([moved[k] for k in range(chips)], down_parts, stream)
        fresh = combined(stream, to_home(blocks), jnp.clip(unit, 0, micro_count - 1))
        return fresh, kept(collected, fresh, jnp.clip(unit, 0, micro_count))

    fresh, collected = lax.fori_loop(1, micro_count + sections - 1, tick, (fresh, collected))
    return collected[None]


def solution(mesh):
    return jax.shard_map(
        local,
        mesh=mesh,
        in_specs=(
            P(None, "expert", None),
            P("pipe", None),
            P("pipe", None, "expert", None),
            P("pipe", None, "expert", None),
            P("pipe", None, "expert", None),
            P("pipe", "expert", None, "tensor"),
            P("pipe", "expert", None, "tensor"),
            P("pipe", "expert", "tensor", None),
        ),
        out_specs=P("pipe", None, "expert", "tensor"),
        check_vma=False,
    )
```

```python
import functools

import jax
import jax.numpy as jnp
from jax import lax
from jax.experimental import pallas as pl
from jax.experimental.pallas import tpu as pltpu
from jax.sharding import PartitionSpec as P

epsilon = 1e-06
bf16 = jnp.bfloat16
f32 = jnp.float32
i32 = jnp.int32
SMEM = pl.BlockSpec(memory_space=pltpu.SMEM)
VMEM = pl.BlockSpec(memory_space=pltpu.VMEM)
HBM = pl.BlockSpec(memory_space=pltpu.HBM)
CHIP_SHIFTS = (2, 1, 3)
RANK_SHIFTS = (2, 1, 3)
BLOCK_PAIRS = ((2, 1), (3, 0))


def kernel_call(body, in_specs, out_shapes, mib, scratch=(), flops=0, moved=0):
    return pl.pallas_call(
        body,
        in_specs=in_specs,
        out_specs=jax.tree.map(lambda _: VMEM, out_shapes),
        out_shape=out_shapes,
        scratch_shapes=list(scratch),
        compiler_params=pltpu.CompilerParams(vmem_limit_bytes=mib << 20),
        cost_estimate=pl.CostEstimate(flops=flops, bytes_accessed=moved, transcendentals=0),
    )


def in_hbm(value):
    return pltpu.with_memory_space_constraint(value, pltpu.HBM)


def shifted(block, axis, distance):
    size = lax.axis_size(axis)
    return lax.ppermute(block, axis, [(i, (i + distance) % size) for i in range(size)])


def core_swap(block):
    size = lax.axis_size("expert")
    return lax.ppermute(block, "expert", [(i, i ^ 1) for i in range(size)])


def onward(block, chips_on):
    sections, groups = lax.axis_size("pipe"), lax.axis_size("expert")
    route = [
        (s * groups + e, ((s + 1) % sections) * groups + (e + 2 * chips_on) % groups)
        for s in range(sections)
        for e in range(groups)
    ]
    return lax.ppermute(block, ("pipe", "expert"), route)


def tables_kernel(sizes, where, info, place, high, low):
    chips, ranks, quarter, capacity = sizes
    tokens = info.shape[3]
    rows = place.shape[2]
    per_pair = ranks * capacity
    chip, core = where[0].astype(f32), where[1].astype(f32)
    across = lax.broadcasted_iota(i32, (tokens, tokens), 1)
    down = lax.broadcasted_iota(i32, (tokens, tokens), 0)
    across_f, down_f = across.astype(f32), down.astype(f32)
    spots = lax.broadcasted_iota(i32, (tokens, rows), 1).astype(f32)

    def column(row):
        return jnp.sum(jnp.where(across == down, row, 0.0), axis=1, keepdims=True)

    for micro in range(info.shape[0]):
        for home in range(2):
            known = info[micro, home]
            id_rows = [known[k : k + 1] for k in range(2)]
            order = known[2:3]
            place_col = jnp.sum(jnp.where(order == down_f, across_f, 0.0), axis=1, keepdims=True)
            place_row = jnp.sum(jnp.where(column(order) == across_f, down_f, 0.0), axis=0, keepdims=True)
            part_col = jnp.floor(place_col * (1.0 / quarter))
            part_row = jnp.floor(place_row * (1.0 / quarter))
            ahead = (part_col == part_row) & (place_row < place_col)
            span = slice(home * tokens, (home + 1) * tokens)
            hot = jnp.zeros((tokens, rows), f32)
            mixed = jnp.zeros((tokens, rows), f32)
            for k in range(2):
                ids = column(id_rows[k])
                same = jnp.where(id_rows[0] == ids, 1.0, 0.0) + jnp.where(id_rows[1] == ids, 1.0, 0.0)
                slot = jnp.sum(jnp.where(ahead, same, 0.0), axis=1, keepdims=True)
                its_chip = jnp.floor(ids * 0.5)
                away = its_chip - chip
                away = jnp.where(away < 0.0, away + chips, away)
                row = away * (2 * per_pair) + home * per_pair + part_col * capacity + slot
                row = jnp.where((slot < capacity) & (ids - 2.0 * its_chip == core), row, -1.0)
                hit = row == spots
                hot = jnp.where(hit, 1.0, hot)
                mixed = jnp.where(hit, column(known[3 + k : 4 + k]), mixed)
            top = mixed.astype(bf16)
            place[micro, span] = hot.astype(bf16)
            high[micro, span] = top
            low[micro, span] = (mixed - top.astype(f32)).astype(bf16)


def dispatch_kernel(which, place, stream, *outs):
    rows = lax.dot_general(
        place[which[0]], stream[...], (((0,), (0,)), ((), ())), preferred_element_type=f32
    )
    count = outs[0].shape[0]
    for k, out in enumerate(outs):
        out[...] = rows[k * count : (k + 1) * count].astype(bf16)


def combine_kernel(which, high, low, *refs):
    *blocks, out = refs
    rows = jnp.concatenate([block[...].astype(f32) for block in blocks]).astype(bf16)
    update = jnp.dot(high[which[0]], rows, preferred_element_type=f32)
    out[...] = update + jnp.dot(low[which[0]], rows, preferred_element_type=f32)


def joined(halves, i):
    return jnp.concatenate([halves[2 * i][...], halves[2 * i + 1][...]]).astype(f32)


def marker_kernel(which, gains, out):
    out[...] = gains[...]


def gate_up_first(early, late, rank, gains, w_gate, w_up, *refs):
    count, downs = len(early), len(early) + len(late)
    w_down, refs = refs[:downs], refs[downs:]
    slices, refs = refs[: 2 * count], refs[2 * count :]
    gate_out, up_out, squares_out, gate_late, up_late, down_out, gate_buf, up_buf, sems, late_sems, down_sems = refs
    width = slices[0].shape[1]
    ranks = w_gate.shape[0] // width

    def pair(k, i, gate_to, up_to, sems):
        start = lax.rem(rank[0] + (ranks - k), ranks) * width
        return [
            pltpu.make_async_copy(w_gate.at[pl.ds(start, width)], gate_to.at[i], sems.at[i, 0]),
            pltpu.make_async_copy(w_up.at[pl.ds(start, width)], up_to.at[i], sems.at[i, 1]),
        ]

    now = [pair(k, i, gate_buf, up_buf, sems) for i, k in enumerate(early)]
    later = [copy for i, k in enumerate(late) for copy in pair(k, i, gate_late, up_late, late_sems)]
    later += [pltpu.make_async_copy(w_down[i], down_out.at[i], down_sems.at[i]) for i in range(downs)]
    for copy in [*now[0], *now[1], *later]:
        copy.start()
    gate, up, squares = 0.0, 0.0, 0.0
    for i, k in enumerate(early):
        wide = joined(slices, i)
        squares = squares + jnp.sum(wide * wide, axis=1, keepdims=True)
        scaled = (wide * gains[k : k + 1]).astype(bf16)
        now[i][0].wait()
        gate = gate + jnp.dot(scaled, gate_buf[i], preferred_element_type=f32)
        now[i][1].wait()
        up = up + jnp.dot(scaled, up_buf[i], preferred_element_type=f32)
    gate_out[...] = gate
    up_out[...] = up
    squares_out[...] = jnp.broadcast_to(squares, squares_out.shape)
    for copy in later:
        copy.wait()


def gate_up_last(late, model_width, gains, gate_late, up_late, gate_in, up_in, squares_in, *refs):
    *slices, hidden = refs
    gate, up, squares = gate_in[...], up_in[...], squares_in[:, :1]
    for i, k in enumerate(late):
        wide = joined(slices, i)
        squares = squares + jnp.sum(wide * wide, axis=1, keepdims=True)
        scaled = (wide * gains[k : k + 1]).astype(bf16)
        gate = gate + jnp.dot(scaled, gate_late[i], preferred_element_type=f32)
        up = up + jnp.dot(scaled, up_late[i], preferred_element_type=f32)
    inv_rms = lax.rsqrt(squares * (1.0 / model_width) + epsilon)
    gate = gate * inv_rms
    hidden[...] = (gate / (1.0 + jnp.exp(-gate)) * (up * inv_rms)).astype(bf16)


def down_first(matrices, own, guest, out):
    out[...] = jnp.dot(own[...], matrices[0], preferred_element_type=f32) + jnp.dot(
        guest[...], matrices[1], preferred_element_type=f32
    )


def down_last(matrices, before, one, other, *outs):
    total = before[...] + jnp.dot(one[...], matrices[2], preferred_element_type=f32)
    total = total + jnp.dot(other[...], matrices[3], preferred_element_type=f32)
    size = outs[0].shape[0]
    for k, piece in enumerate(outs):
        piece[...] = total[k * size : (k + 1) * size].astype(bf16)


def local(tokens, gains, route_ids, route_weights, picks, w_gate, w_up, w_down):
    micro_count, local_tokens, model_width = tokens.shape
    route_count = route_ids.shape[3]
    ranks = lax.axis_size("tensor")
    groups = lax.axis_size("expert")
    sections = lax.axis_size("pipe")
    chips = groups // 2
    quarter = local_tokens // ranks
    capacity = 4 * quarter * route_count // (3 * groups)
    width = model_width // ranks
    hidden_width = w_gate.shape[3]
    per_chip = 2 * ranks * capacity
    rows = chips * per_chip
    section = lax.axis_index("pipe")
    rank = lax.axis_index("tensor")
    group = lax.axis_index("expert")
    chip, core = group // 2, group % 2
    gate_matrix, up_matrix, down_matrix = w_gate[0, 0], w_up[0, 0], w_down[0, 0]

    def slice_at(value, index, dim):
        return lax.dynamic_slice_in_dim(value, ((index + ranks) % ranks) * width, width, dim)

    def by_core(mine, guest, dim):
        first = jnp.where(core == 0, mine, guest)
        second = jnp.where(core == 0, guest, mine)
        return jnp.concatenate([first, second], axis=dim)

    def shape(*dims, kind=bf16):
        return pltpu.VMEM(dims, kind)

    down_parts = {k: shifted(slice_at(down_matrix, rank + k, 1), "tensor", k) for k in RANK_SHIFTS}
    down_parts[0] = slice_at(down_matrix, rank, 1)

    info = jnp.concatenate(
        [route_ids[0].transpose(0, 2, 1).astype(f32), picks[0].astype(f32), route_weights[0].transpose(0, 2, 1)],
        axis=1,
    )[:, None]
    info = by_core(info, core_swap(info), 1)
    where = jnp.stack([chip, core]).astype(i32)
    table = shape(micro_count, 2 * local_tokens, rows)
    tables = kernel_call(
        functools.partial(tables_kernel, (chips, ranks, quarter, capacity)), (SMEM, VMEM), (table, table, table), 8
    )
    first_place, high, low = tables(where, info)

    own_slice = lax.dynamic_slice_in_dim(tokens, rank * width, width, 2)
    entering = by_core(own_slice, core_swap(own_slice), 1)

    dispatch = kernel_call(dispatch_kernel, (SMEM, VMEM, VMEM), (shape(per_chip, width),) * chips, 8, flops=10**9)
    combine = kernel_call(
        combine_kernel, (SMEM, VMEM, VMEM) + (VMEM,) * chips, shape(2 * local_tokens, width, kind=f32), 8, flops=10**9
    )
    early, late = (0, 1), (3, 2)
    gate_up_a = kernel_call(
        functools.partial(gate_up_first, early, late),
        (SMEM, VMEM, HBM, HBM) + (HBM,) * ranks + (VMEM,) * 4,
        (shape(rows, hidden_width, kind=f32),) * 2
        + (shape(rows, 128, kind=f32),)
        + (shape(2, width, hidden_width),) * 2
        + (shape(ranks, hidden_width, width),),
        24,
        [pltpu.VMEM((2, width, hidden_width), bf16)] * 2
        + [pltpu.SemaphoreType.DMA((2, 2)), pltpu.SemaphoreType.DMA((2, 2)), pltpu.SemaphoreType.DMA((ranks,))],
        flops=3 * 10**9,
    )
    gate_up_b = kernel_call(
        functools.partial(gate_up_last, late, model_width), (VMEM,) * 10, shape(rows, hidden_width), 16, flops=10**9
    )
    down_a = kernel_call(down_first, (VMEM,) * 3, shape(rows, width, kind=f32), 16, flops=5 * 10**8)
    down_b = kernel_call(down_last, (VMEM,) * 4, (shape(per_chip, width),) * chips, 16, flops=5 * 10**8)

    rank_word = rank.reshape(1).astype(i32)
    gain_parts = jnp.concatenate([slice_at(gains, rank - k, 1) for k in range(ranks)])

    marker = kernel_call(marker_kernel, (SMEM, VMEM), shape(ranks, width, kind=f32), 4, flops=10**6)

    def expert_work(blocks, down_parts, also, gain_parts):
        halves = [jnp.concatenate([blocks[k] for k in pair]) for pair in BLOCK_PAIRS]
        slices = {k: [shifted(half, "tensor", k) for half in halves] for k in RANK_SHIFTS}
        slices[0] = halves
        weights = [in_hbm(value) for value in (gate_matrix, up_matrix, *(down_parts[k] for k in (*early, *late)))]
        gate, up, squares, gate_late, up_late, matrices = gate_up_a(
            rank_word, gain_parts, *weights, *(half for k in early for half in slices[k])
        )
        hidden = gate_up_b(gain_parts, gate_late, up_late, gate, up, squares, *(half for k in late for half in slices[k]))
        hidden, also = lax.optimization_barrier((hidden, also))
        hiddens = {k: shifted(hidden, "tensor", k) for k in RANK_SHIFTS}
        hiddens[0] = hidden
        total = down_a(matrices, *(hiddens[k] for k in early))
        outs = down_b(matrices, total, *(hiddens[k] for k in late))
        order = [k for pair in BLOCK_PAIRS for k in pair]
        return [outs[order.index(k)] for k in range(chips)], also

    def to_home(blocks):
        back = {k: shifted(blocks[k], "expert", groups - 2 * k) for k in CHIP_SHIFTS}
        back[0] = blocks[0]
        return [back[k] for k in range(chips)]

    def combined(stream, blocks, which):
        update = combine(which.reshape(1), high, low, *blocks)
        return (stream.astype(f32) + (update + core_swap(update))).astype(bf16)

    def kept(collected, fresh, spot):
        own = lax.dynamic_slice_in_dim(fresh, core * local_tokens, local_tokens)[None]
        held = lax.dynamic_slice_in_dim(collected, jnp.minimum(spot, micro_count - 1), 1)
        own = jnp.where(spot < micro_count, own, held)
        return lax.dynamic_update_slice_in_dim(collected, own, jnp.minimum(spot, micro_count - 1), 0)

    outgoing = dispatch(jnp.zeros(1, i32), first_place, entering[0])
    moved = {k: shifted(outgoing[k], "expert", 2 * k) for k in CHIP_SHIFTS}
    moved[0] = outgoing[0]

    next_info = shifted(info, "pipe", sections - 1)
    place = tables(where, next_info)[0]

    blocks, stream = expert_work([moved[k] for k in range(chips)], down_parts, entering[0], gain_parts)
    fresh = combined(stream, to_home(blocks), jnp.zeros((), i32))
    collected = kept(jnp.zeros((micro_count, local_tokens, width), bf16), fresh, 0)
    fresh = jnp.where(section == sections - 1, entering[1], fresh)

    def tick(index, carry):
        fresh, collected = carry
        unit = index - section
        leaving = jnp.where(section == sections - 1, 1, jnp.clip(unit - 1, 0, micro_count - 1))
        outgoing = dispatch(leaving.reshape(1), place, fresh)
        moved = {k: onward(outgoing[k], k) for k in (*CHIP_SHIFTS, 0)}
        stream = shifted(fresh, "pipe", 1)
        gains_here = marker(index.reshape(1), gain_parts)
        gains_here = marker(index.reshape(1), gains_here)
        blocks, stream = expert_work([moved[k] for k in range(chips)], down_parts, stream, gains_here)
        fresh = combined(stream, to_home(blocks), jnp.clip(unit, 0, micro_count - 1))
        return fresh, kept(collected, fresh, jnp.clip(unit, 0, micro_count))

    fresh, collected = lax.fori_loop(1, micro_count + sections - 1, tick, (fresh, collected))
    return collected[None]


def solution(mesh):
    return jax.shard_map(
        local,
        mesh=mesh,
        in_specs=(
            P(None, "expert", None),
            P("pipe", None),
            P("pipe", None, "expert", None),
            P("pipe", None, "expert", None),
            P("pipe", None, "expert", None),
            P("pipe", "expert", None, "tensor"),
            P("pipe", "expert", None, "tensor"),
            P("pipe", "expert", "tensor", None),
        ),
        out_specs=P("pipe", None, "expert", "tensor"),
        check_vma=False,
    )
```

```python
import functools

import jax
import jax.numpy as jnp
from jax import lax
from jax.experimental import pallas as pl
from jax.experimental.pallas import tpu as pltpu
from jax.sharding import PartitionSpec as P

epsilon = 1e-06
bf16 = jnp.bfloat16
f32 = jnp.float32
i32 = jnp.int32
SMEM = pl.BlockSpec(memory_space=pltpu.SMEM)
VMEM = pl.BlockSpec(memory_space=pltpu.VMEM)
HBM = pl.BlockSpec(memory_space=pltpu.HBM)
CHIP_SHIFTS = (2, 1, 3)
RANK_SHIFTS = (2, 1, 3)
BLOCK_PAIRS = ((2, 1), (3, 0))


def kernel_call(body, in_specs, out_shapes, mib, scratch=(), flops=0, moved=0):
    return pl.pallas_call(
        body,
        in_specs=in_specs,
        out_specs=jax.tree.map(lambda _: VMEM, out_shapes),
        out_shape=out_shapes,
        scratch_shapes=list(scratch),
        compiler_params=pltpu.CompilerParams(vmem_limit_bytes=mib << 20),
        cost_estimate=pl.CostEstimate(flops=flops, bytes_accessed=moved, transcendentals=0),
    )


def in_hbm(value):
    return pltpu.with_memory_space_constraint(value, pltpu.HBM)


def shifted(block, axis, distance):
    size = lax.axis_size(axis)
    return lax.ppermute(block, axis, [(i, (i + distance) % size) for i in range(size)])


def core_swap(block):
    size = lax.axis_size("expert")
    return lax.ppermute(block, "expert", [(i, i ^ 1) for i in range(size)])


def onward(block, chips_on):
    sections, groups = lax.axis_size("pipe"), lax.axis_size("expert")
    route = [
        (s * groups + e, ((s + 1) % sections) * groups + (e + 2 * chips_on) % groups)
        for s in range(sections)
        for e in range(groups)
    ]
    return lax.ppermute(block, ("pipe", "expert"), route)


def tables_kernel(sizes, where, info, place, high, low):
    chips, ranks, quarter, capacity = sizes
    tokens = info.shape[3]
    rows = place.shape[2]
    per_pair = ranks * capacity
    chip, core = where[0].astype(f32), where[1].astype(f32)
    across = lax.broadcasted_iota(i32, (tokens, tokens), 1)
    down = lax.broadcasted_iota(i32, (tokens, tokens), 0)
    across_f, down_f = across.astype(f32), down.astype(f32)
    spots = lax.broadcasted_iota(i32, (tokens, rows), 1).astype(f32)

    def column(row):
        return jnp.sum(jnp.where(across == down, row, 0.0), axis=1, keepdims=True)

    for micro in range(info.shape[0]):
        for home in range(2):
            known = info[micro, home]
            id_rows = [known[k : k + 1] for k in range(2)]
            order = known[2:3]
            place_col = jnp.sum(jnp.where(order == down_f, across_f, 0.0), axis=1, keepdims=True)
            place_row = jnp.sum(jnp.where(column(order) == across_f, down_f, 0.0), axis=0, keepdims=True)
            part_col = jnp.floor(place_col * (1.0 / quarter))
            part_row = jnp.floor(place_row * (1.0 / quarter))
            ahead = (part_col == part_row) & (place_row < place_col)
            span = slice(home * tokens, (home + 1) * tokens)
            hot = jnp.zeros((tokens, rows), f32)
            mixed = jnp.zeros((tokens, rows), f32)
            for k in range(2):
                ids = column(id_rows[k])
                same = jnp.where(id_rows[0] == ids, 1.0, 0.0) + jnp.where(id_rows[1] == ids, 1.0, 0.0)
                slot = jnp.sum(jnp.where(ahead, same, 0.0), axis=1, keepdims=True)
                its_chip = jnp.floor(ids * 0.5)
                away = its_chip - chip
                away = jnp.where(away < 0.0, away + chips, away)
                row = away * (2 * per_pair) + home * per_pair + part_col * capacity + slot
                row = jnp.where((slot < capacity) & (ids - 2.0 * its_chip == core), row, -1.0)
                hit = row == spots
                hot = jnp.where(hit, 1.0, hot)
                mixed = jnp.where(hit, column(known[3 + k : 4 + k]), mixed)
            top = mixed.astype(bf16)
            place[micro, span] = hot.astype(bf16)
            high[micro, span] = top
            low[micro, span] = (mixed - top.astype(f32)).astype(bf16)


def dispatch_kernel(which, place, stream, *outs):
    rows = lax.dot_general(
        place[which[0]], stream[...], (((0,), (0,)), ((), ())), preferred_element_type=f32
    )
    count = outs[0].shape[0]
    for k, out in enumerate(outs):
        out[...] = rows[k * count : (k + 1) * count].astype(bf16)


def combine_kernel(which, high, low, *refs):
    *blocks, out, swapped = refs
    rows = jnp.concatenate([block[...].astype(f32) for block in blocks]).astype(bf16)
    update = jnp.dot(high[which[0]], rows, preferred_element_type=f32)
    update = update + jnp.dot(low[which[0]], rows, preferred_element_type=f32)
    out[...] = update
    swapped[...] = update.astype(bf16)


def joined(halves, i):
    return jnp.concatenate([halves[2 * i][...], halves[2 * i + 1][...]]).astype(f32)


def marker_kernel(which, gains, out):
    out[...] = gains[...]


def gate_up_first(early, late, rank, gains, w_gate, w_up, *refs):
    count, downs = len(early), len(early) + len(late)
    w_down, refs = refs[:downs], refs[downs:]
    slices, refs = refs[: 2 * count], refs[2 * count :]
    gate_out, up_out, squares_out, gate_late, up_late, down_out, gate_buf, up_buf, sems, late_sems, down_sems = refs
    width = slices[0].shape[1]
    ranks = w_gate.shape[0] // width

    def pair(k, i, gate_to, up_to, sems):
        start = lax.rem(rank[0] + (ranks - k), ranks) * width
        return [
            pltpu.make_async_copy(w_gate.at[pl.ds(start, width)], gate_to.at[i], sems.at[i, 0]),
            pltpu.make_async_copy(w_up.at[pl.ds(start, width)], up_to.at[i], sems.at[i, 1]),
        ]

    now = [pair(k, i, gate_buf, up_buf, sems) for i, k in enumerate(early)]
    later = [copy for i, k in enumerate(late) for copy in pair(k, i, gate_late, up_late, late_sems)]
    later += [pltpu.make_async_copy(w_down[i], down_out.at[i], down_sems.at[i]) for i in range(downs)]
    for copy in [copy for pieces in now for copy in pieces] + later:
        copy.start()
    gate, up, squares = 0.0, 0.0, 0.0
    for i, k in enumerate(early):
        wide = joined(slices, i)
        squares = squares + jnp.sum(wide * wide, axis=1, keepdims=True)
        scaled = (wide * gains[k : k + 1]).astype(bf16)
        now[i][0].wait()
        gate = gate + jnp.dot(scaled, gate_buf[i], preferred_element_type=f32)
        now[i][1].wait()
        up = up + jnp.dot(scaled, up_buf[i], preferred_element_type=f32)
    gate_out[...] = gate
    up_out[...] = up
    squares_out[...] = jnp.broadcast_to(squares, squares_out.shape)
    for copy in later:
        copy.wait()


def gate_up_last(late, model_width, gains, gate_late, up_late, gate_in, up_in, squares_in, *refs):
    *slices, hidden = refs
    gate, up, squares = gate_in[...], up_in[...], squares_in[:, :1]
    for i, k in enumerate(late):
        wide = joined(slices, i)
        squares = squares + jnp.sum(wide * wide, axis=1, keepdims=True)
        scaled = (wide * gains[k : k + 1]).astype(bf16)
        gate = gate + jnp.dot(scaled, gate_late[i], preferred_element_type=f32)
        up = up + jnp.dot(scaled, up_late[i], preferred_element_type=f32)
    inv_rms = lax.rsqrt(squares * (1.0 / model_width) + epsilon)
    gate = gate * inv_rms
    hidden[...] = (gate / (1.0 + jnp.exp(-gate)) * (up * inv_rms)).astype(bf16)


def down_first(matrices, own, guest, out):
    out[...] = jnp.dot(own[...], matrices[0], preferred_element_type=f32) + jnp.dot(
        guest[...], matrices[1], preferred_element_type=f32
    )


def down_last(matrices, before, one, other, *outs):
    total = before[...] + jnp.dot(one[...], matrices[2], preferred_element_type=f32)
    total = total + jnp.dot(other[...], matrices[3], preferred_element_type=f32)
    size = outs[0].shape[0]
    for k, piece in enumerate(outs):
        piece[...] = total[k * size : (k + 1) * size].astype(bf16)


def local(tokens, gains, route_ids, route_weights, picks, w_gate, w_up, w_down):
    micro_count, local_tokens, model_width = tokens.shape
    route_count = route_ids.shape[3]
    ranks = lax.axis_size("tensor")
    groups = lax.axis_size("expert")
    sections = lax.axis_size("pipe")
    chips = groups // 2
    quarter = local_tokens // ranks
    capacity = 4 * quarter * route_count // (3 * groups)
    width = model_width // ranks
    hidden_width = w_gate.shape[3]
    per_chip = 2 * ranks * capacity
    rows = chips * per_chip
    section = lax.axis_index("pipe")
    rank = lax.axis_index("tensor")
    group = lax.axis_index("expert")
    chip, core = group // 2, group % 2
    gate_matrix, up_matrix, down_matrix = w_gate[0, 0], w_up[0, 0], w_down[0, 0]

    def slice_at(value, index, dim):
        return lax.dynamic_slice_in_dim(value, ((index + ranks) % ranks) * width, width, dim)

    def by_core(mine, guest, dim):
        first = jnp.where(core == 0, mine, guest)
        second = jnp.where(core == 0, guest, mine)
        return jnp.concatenate([first, second], axis=dim)

    def shape(*dims, kind=bf16):
        return pltpu.VMEM(dims, kind)

    down_parts = {k: shifted(slice_at(down_matrix, rank + k, 1), "tensor", k) for k in RANK_SHIFTS}
    down_parts[0] = slice_at(down_matrix, rank, 1)

    info = jnp.concatenate(
        [route_ids[0].transpose(0, 2, 1).astype(f32), picks[0].astype(f32), route_weights[0].transpose(0, 2, 1)],
        axis=1,
    )[:, None]
    info = by_core(info, core_swap(info), 1)
    where = jnp.stack([chip, core]).astype(i32)
    table = shape(micro_count, 2 * local_tokens, rows)
    tables = kernel_call(
        functools.partial(tables_kernel, (chips, ranks, quarter, capacity)), (SMEM, VMEM), (table, table, table), 8
    )
    first_place, high, low = tables(where, info)

    own_slice = lax.dynamic_slice_in_dim(tokens, rank * width, width, 2)
    entering = by_core(own_slice, core_swap(own_slice), 1)

    dispatch = kernel_call(dispatch_kernel, (SMEM, VMEM, VMEM), (shape(per_chip, width),) * chips, 8, flops=10**9)
    combine = kernel_call(
        combine_kernel,
        (SMEM, VMEM, VMEM) + (VMEM,) * chips,
        (shape(2 * local_tokens, width, kind=f32), shape(2 * local_tokens, width)),
        8,
        flops=10**9,
    )
    early, late = (0,), (1, 3, 2)
    order = (0, 1, 3, 2)
    gate_up_a = kernel_call(
        functools.partial(gate_up_first, early, late),
        (SMEM, VMEM, HBM, HBM) + (HBM,) * ranks + (VMEM,) * 2,
        (shape(rows, hidden_width, kind=f32),) * 2
        + (shape(rows, 128, kind=f32),)
        + (shape(len(late), width, hidden_width),) * 2
        + (shape(ranks, hidden_width, width),),
        24,
        [pltpu.VMEM((len(early), width, hidden_width), bf16)] * 2
        + [pltpu.SemaphoreType.DMA((len(part), 2)) for part in (early, late)]
        + [pltpu.SemaphoreType.DMA((ranks,))],
        flops=3 * 10**9,
    )
    gate_up_b = kernel_call(
        functools.partial(gate_up_last, late, model_width),
        (VMEM,) * (6 + 2 * len(late)),
        shape(rows, hidden_width),
        16,
        flops=10**9,
    )
    down_a = kernel_call(down_first, (VMEM,) * 3, shape(rows, width, kind=f32), 16, flops=5 * 10**8)
    down_b = kernel_call(down_last, (VMEM,) * 4, (shape(per_chip, width),) * chips, 16, flops=5 * 10**8)

    rank_word = rank.reshape(1).astype(i32)
    gain_parts = jnp.concatenate([slice_at(gains, rank - k, 1) for k in range(ranks)])

    marker = kernel_call(marker_kernel, (SMEM, VMEM), shape(ranks, width, kind=f32), 4, flops=10**6)

    def expert_work(blocks, down_parts, also, gain_parts):
        halves = [jnp.concatenate([blocks[k] for k in pair]) for pair in BLOCK_PAIRS]
        slices = {k: [shifted(half, "tensor", k) for half in halves] for k in RANK_SHIFTS}
        slices[0] = halves
        weights = [in_hbm(value) for value in (gate_matrix, up_matrix, *(down_parts[k] for k in order))]
        gate, up, squares, gate_late, up_late, matrices = gate_up_a(
            rank_word, gain_parts, *weights, *(half for k in early for half in slices[k])
        )
        hidden = gate_up_b(gain_parts, gate_late, up_late, gate, up, squares, *(half for k in late for half in slices[k]))
        hidden, also = lax.optimization_barrier((hidden, also))
        hiddens = {k: shifted(hidden, "tensor", k) for k in RANK_SHIFTS}
        hiddens[0] = hidden
        total = down_a(matrices, *(hiddens[k] for k in order[:2]))
        outs = down_b(matrices, total, *(hiddens[k] for k in order[2:]))
        blocks_out = [k for pair in BLOCK_PAIRS for k in pair]
        return [outs[blocks_out.index(k)] for k in range(chips)], also

    def to_home(blocks):
        back = {k: shifted(blocks[k], "expert", groups - 2 * k) for k in CHIP_SHIFTS}
        back[0] = blocks[0]
        return [back[k] for k in range(chips)]

    def combined(stream, blocks, which):
        update, swapped = combine(which.reshape(1), high, low, *blocks)
        return (stream.astype(f32) + (update + core_swap(swapped).astype(f32))).astype(bf16)

    def kept(collected, fresh, spot):
        own = lax.dynamic_slice_in_dim(fresh, core * local_tokens, local_tokens)[None]
        held = lax.dynamic_slice_in_dim(collected, jnp.minimum(spot, micro_count - 1), 1)
        own = jnp.where(spot < micro_count, own, held)
        return lax.dynamic_update_slice_in_dim(collected, own, jnp.minimum(spot, micro_count - 1), 0)

    outgoing = dispatch(jnp.zeros(1, i32), first_place, entering[0])
    moved = {k: shifted(outgoing[k], "expert", 2 * k) for k in CHIP_SHIFTS}
    moved[0] = outgoing[0]

    next_info = shifted(info, "pipe", sections - 1)
    place = tables(where, next_info)[0]

    blocks, stream = expert_work([moved[k] for k in range(chips)], down_parts, entering[0], gain_parts)
    fresh = combined(stream, to_home(blocks), jnp.zeros((), i32))
    collected = kept(jnp.zeros((micro_count, local_tokens, width), bf16), fresh, 0)
    fresh = jnp.where(section == sections - 1, entering[1], fresh)

    def tick(index, carry):
        fresh, collected = carry
        unit = index - section
        leaving = jnp.where(section == sections - 1, 1, jnp.clip(unit - 1, 0, micro_count - 1))
        outgoing = dispatch(leaving.reshape(1), place, fresh)
        moved = {k: onward(outgoing[k], k) for k in (*CHIP_SHIFTS, 0)}
        stream = shifted(fresh, "pipe", 1)
        gains_here = marker(index.reshape(1), gain_parts)
        blocks, stream = expert_work([moved[k] for k in range(chips)], down_parts, stream, gains_here)
        fresh = combined(stream, to_home(blocks), jnp.clip(unit, 0, micro_count - 1))
        return fresh, kept(collected, fresh, jnp.clip(unit, 0, micro_count))

    fresh, collected = lax.fori_loop(1, micro_count + sections - 1, tick, (fresh, collected))
    return collected[None]


def solution(mesh):
    return jax.shard_map(
        local,
        mesh=mesh,
        in_specs=(
            P(None, "expert", None),
            P("pipe", None),
            P("pipe", None, "expert", None),
            P("pipe", None, "expert", None),
            P("pipe", None, "expert", None),
            P("pipe", "expert", None, "tensor"),
            P("pipe", "expert", None, "tensor"),
            P("pipe", "expert", "tensor", None),
        ),
        out_specs=P("pipe", None, "expert", "tensor"),
        check_vma=False,
    )
```

```python
import functools

import jax
import jax.numpy as jnp
from jax import lax
from jax.experimental import pallas as pl
from jax.experimental.pallas import tpu as pltpu
from jax.sharding import PartitionSpec as P

epsilon = 1e-06
bf16 = jnp.bfloat16
f32 = jnp.float32
i32 = jnp.int32
SMEM = pl.BlockSpec(memory_space=pltpu.SMEM)
VMEM = pl.BlockSpec(memory_space=pltpu.VMEM)
HBM = pl.BlockSpec(memory_space=pltpu.HBM)
CHIP_SHIFTS = (2, 1, 3)
RANK_SHIFTS = (2, 1, 3)
BLOCK_PAIRS = ((2, 1), (3, 0))


def kernel_call(body, in_specs, out_shapes, mib, scratch=(), flops=0, moved=0):
    return pl.pallas_call(
        body,
        in_specs=in_specs,
        out_specs=jax.tree.map(lambda _: VMEM, out_shapes),
        out_shape=out_shapes,
        scratch_shapes=list(scratch),
        compiler_params=pltpu.CompilerParams(vmem_limit_bytes=mib << 20),
        cost_estimate=pl.CostEstimate(flops=flops, bytes_accessed=moved, transcendentals=0),
    )


def in_hbm(value):
    return pltpu.with_memory_space_constraint(value, pltpu.HBM)


def shifted(block, axis, distance):
    size = lax.axis_size(axis)
    return lax.ppermute(block, axis, [(i, (i + distance) % size) for i in range(size)])


def core_swap(block):
    size = lax.axis_size("expert")
    return lax.ppermute(block, "expert", [(i, i ^ 1) for i in range(size)])


def onward(block, chips_on):
    sections, groups = lax.axis_size("pipe"), lax.axis_size("expert")
    route = [
        (s * groups + e, ((s + 1) % sections) * groups + (e + 2 * chips_on) % groups)
        for s in range(sections)
        for e in range(groups)
    ]
    return lax.ppermute(block, ("pipe", "expert"), route)


def tables_kernel(sizes, where, info, place, high, low):
    chips, ranks, quarter, capacity = sizes
    tokens = info.shape[3]
    rows = place.shape[2]
    per_pair = ranks * capacity
    chip, core = where[0].astype(f32), where[1].astype(f32)
    across = lax.broadcasted_iota(i32, (tokens, tokens), 1)
    down = lax.broadcasted_iota(i32, (tokens, tokens), 0)
    across_f, down_f = across.astype(f32), down.astype(f32)
    spots = lax.broadcasted_iota(i32, (tokens, rows), 1).astype(f32)

    def column(row):
        return jnp.sum(jnp.where(across == down, row, 0.0), axis=1, keepdims=True)

    for micro in range(info.shape[0]):
        for home in range(2):
            known = info[micro, home]
            id_rows = [known[k : k + 1] for k in range(2)]
            order = known[2:3]
            place_col = jnp.sum(jnp.where(order == down_f, across_f, 0.0), axis=1, keepdims=True)
            place_row = jnp.sum(jnp.where(column(order) == across_f, down_f, 0.0), axis=0, keepdims=True)
            part_col = jnp.floor(place_col * (1.0 / quarter))
            part_row = jnp.floor(place_row * (1.0 / quarter))
            ahead = (part_col == part_row) & (place_row < place_col)
            span = slice(home * tokens, (home + 1) * tokens)
            hot = jnp.zeros((tokens, rows), f32)
            mixed = jnp.zeros((tokens, rows), f32)
            for k in range(2):
                ids = column(id_rows[k])
                same = jnp.where(id_rows[0] == ids, 1.0, 0.0) + jnp.where(id_rows[1] == ids, 1.0, 0.0)
                slot = jnp.sum(jnp.where(ahead, same, 0.0), axis=1, keepdims=True)
                its_chip = jnp.floor(ids * 0.5)
                away = its_chip - chip
                away = jnp.where(away < 0.0, away + chips, away)
                row = away * (2 * per_pair) + home * per_pair + part_col * capacity + slot
                row = jnp.where((slot < capacity) & (ids - 2.0 * its_chip == core), row, -1.0)
                hit = row == spots
                hot = jnp.where(hit, 1.0, hot)
                mixed = jnp.where(hit, column(known[3 + k : 4 + k]), mixed)
            top = mixed.astype(bf16)
            place[micro, span] = hot.astype(bf16)
            high[micro, span] = top
            low[micro, span] = (mixed - top.astype(f32)).astype(bf16)


def dispatch_kernel(which, place, stream, *outs):
    rows = lax.dot_general(
        place[which[0]], stream[...], (((0,), (0,)), ((), ())), preferred_element_type=f32
    )
    count = outs[0].shape[0]
    for k, out in enumerate(outs):
        out[...] = rows[k * count : (k + 1) * count].astype(bf16)


def combine_kernel(which, high, low, *refs):
    *blocks, out, swapped = refs
    rows = jnp.concatenate([block[...].astype(f32) for block in blocks]).astype(bf16)
    update = jnp.dot(high[which[0]], rows, preferred_element_type=f32)
    update = update + jnp.dot(low[which[0]], rows, preferred_element_type=f32)
    out[...] = update
    swapped[...] = update.astype(bf16)


def joined(halves, i):
    return jnp.concatenate([halves[2 * i][...], halves[2 * i + 1][...]]).astype(f32)


def marker_kernel(which, gains, out):
    out[...] = gains[...]


def gate_up_first(early, late, rank, gains, w_gate, w_up, *refs):
    count, downs = len(early), len(early) + len(late)
    w_down, refs = refs[:downs], refs[downs:]
    slices, refs = refs[: 2 * count], refs[2 * count :]
    gate_out, up_out, squares_out, gate_late, up_late, down_out, gate_buf, up_buf, sems, late_sems, down_sems = refs
    width = slices[0].shape[1]
    ranks = w_gate.shape[0] // width

    def pair(k, i, gate_to, up_to, sems):
        start = lax.rem(rank[0] + (ranks - k), ranks) * width
        return [
            pltpu.make_async_copy(w_gate.at[pl.ds(start, width)], gate_to.at[i], sems.at[i, 0]),
            pltpu.make_async_copy(w_up.at[pl.ds(start, width)], up_to.at[i], sems.at[i, 1]),
        ]

    now = [pair(k, i, gate_buf, up_buf, sems) for i, k in enumerate(early)]
    later = [copy for i, k in enumerate(late) for copy in pair(k, i, gate_late, up_late, late_sems)]
    later += [pltpu.make_async_copy(w_down[i], down_out.at[i], down_sems.at[i]) for i in range(downs)]
    for copy in [copy for pieces in now for copy in pieces] + later:
        copy.start()
    gate, up, squares = 0.0, 0.0, 0.0
    for i, k in enumerate(early):
        wide = joined(slices, i)
        squares = squares + jnp.sum(wide * wide, axis=1, keepdims=True)
        scaled = (wide * gains[k : k + 1]).astype(bf16)
        now[i][0].wait()
        gate = gate + jnp.dot(scaled, gate_buf[i], preferred_element_type=f32)
        now[i][1].wait()
        up = up + jnp.dot(scaled, up_buf[i], preferred_element_type=f32)
    gate_out[...] = gate
    up_out[...] = up
    squares_out[...] = jnp.broadcast_to(squares, squares_out.shape)
    for copy in later:
        copy.wait()


def gate_up_last(late, model_width, gains, gate_late, up_late, gate_in, up_in, squares_in, *refs):
    *slices, hidden = refs
    gate, up, squares = gate_in[...], up_in[...], squares_in[:, :1]
    for i, k in enumerate(late):
        wide = joined(slices, i)
        squares = squares + jnp.sum(wide * wide, axis=1, keepdims=True)
        scaled = (wide * gains[k : k + 1]).astype(bf16)
        gate = gate + jnp.dot(scaled, gate_late[i], preferred_element_type=f32)
        up = up + jnp.dot(scaled, up_late[i], preferred_element_type=f32)
    inv_rms = lax.rsqrt(squares * (1.0 / model_width) + epsilon)
    gate = gate * inv_rms
    hidden[...] = (gate / (1.0 + jnp.exp(-gate)) * (up * inv_rms)).astype(bf16)


def down_first(matrices, own, out):
    out[...] = jnp.dot(own[...], matrices[0], preferred_element_type=f32)


def down_last(matrices, before, *refs):
    parts, outs = refs[:3], refs[3:]
    total = before[...]
    for i, part in enumerate(parts, 1):
        total = total + jnp.dot(part[...], matrices[i], preferred_element_type=f32)
    size = outs[0].shape[0]
    for k, piece in enumerate(outs):
        piece[...] = total[k * size : (k + 1) * size].astype(bf16)


def local(tokens, gains, route_ids, route_weights, picks, w_gate, w_up, w_down):
    micro_count, local_tokens, model_width = tokens.shape
    route_count = route_ids.shape[3]
    ranks = lax.axis_size("tensor")
    groups = lax.axis_size("expert")
    sections = lax.axis_size("pipe")
    chips = groups // 2
    quarter = local_tokens // ranks
    capacity = 4 * quarter * route_count // (3 * groups)
    width = model_width // ranks
    hidden_width = w_gate.shape[3]
    per_chip = 2 * ranks * capacity
    rows = chips * per_chip
    section = lax.axis_index("pipe")
    rank = lax.axis_index("tensor")
    group = lax.axis_index("expert")
    chip, core = group // 2, group % 2
    gate_matrix, up_matrix, down_matrix = w_gate[0, 0], w_up[0, 0], w_down[0, 0]

    def slice_at(value, index, dim):
        return lax.dynamic_slice_in_dim(value, ((index + ranks) % ranks) * width, width, dim)

    def by_core(mine, guest, dim):
        first = jnp.where(core == 0, mine, guest)
        second = jnp.where(core == 0, guest, mine)
        return jnp.concatenate([first, second], axis=dim)

    def shape(*dims, kind=bf16):
        return pltpu.VMEM(dims, kind)

    down_parts = {k: shifted(slice_at(down_matrix, rank + k, 1), "tensor", k) for k in RANK_SHIFTS}
    down_parts[0] = slice_at(down_matrix, rank, 1)

    info = jnp.concatenate(
        [route_ids[0].transpose(0, 2, 1).astype(f32), picks[0].astype(f32), route_weights[0].transpose(0, 2, 1)],
        axis=1,
    )[:, None]
    info = by_core(info, core_swap(info), 1)
    where = jnp.stack([chip, core]).astype(i32)
    table = shape(micro_count, 2 * local_tokens, rows)
    tables = kernel_call(
        functools.partial(tables_kernel, (chips, ranks, quarter, capacity)), (SMEM, VMEM), (table, table, table), 8
    )
    first_place, high, low = tables(where, info)

    own_slice = lax.dynamic_slice_in_dim(tokens, rank * width, width, 2)
    entering = by_core(own_slice, core_swap(own_slice), 1)

    dispatch = kernel_call(dispatch_kernel, (SMEM, VMEM, VMEM), (shape(per_chip, width),) * chips, 8, flops=10**9)
    combine = kernel_call(
        combine_kernel,
        (SMEM, VMEM, VMEM) + (VMEM,) * chips,
        (shape(2 * local_tokens, width, kind=f32), shape(2 * local_tokens, width)),
        8,
        flops=10**9,
    )
    early, late = (0,), (1, 3, 2)
    order = (0, 1, 3, 2)
    gate_up_a = kernel_call(
        functools.partial(gate_up_first, early, late),
        (SMEM, VMEM, HBM, HBM) + (HBM,) * ranks + (VMEM,) * 2,
        (shape(rows, hidden_width, kind=f32),) * 2
        + (shape(rows, 128, kind=f32),)
        + (shape(len(late), width, hidden_width),) * 2
        + (shape(ranks, hidden_width, width),),
        24,
        [pltpu.VMEM((len(early), width, hidden_width), bf16)] * 2
        + [pltpu.SemaphoreType.DMA((len(part), 2)) for part in (early, late)]
        + [pltpu.SemaphoreType.DMA((ranks,))],
        flops=3 * 10**9,
    )
    gate_up_b = kernel_call(
        functools.partial(gate_up_last, late, model_width),
        (VMEM,) * (6 + 2 * len(late)),
        shape(rows, hidden_width),
        16,
        flops=10**9,
    )
    down_a = kernel_call(down_first, (VMEM,) * 2, shape(rows, width, kind=f32), 16, flops=5 * 10**8)
    down_b = kernel_call(down_last, (VMEM,) * 5, (shape(per_chip, width),) * chips, 16, flops=5 * 10**8)

    rank_word = rank.reshape(1).astype(i32)
    gain_parts = jnp.concatenate([slice_at(gains, rank - k, 1) for k in range(ranks)])

    marker = kernel_call(marker_kernel, (SMEM, VMEM), shape(ranks, width, kind=f32), 4, flops=10**6)

    def expert_work(blocks, down_parts, also, gain_parts):
        halves = [jnp.concatenate([blocks[k] for k in pair]) for pair in BLOCK_PAIRS]
        slices = {k: [shifted(half, "tensor", k) for half in halves] for k in RANK_SHIFTS}
        slices[0] = halves
        weights = [in_hbm(value) for value in (gate_matrix, up_matrix, *(down_parts[k] for k in order))]
        gate, up, squares, gate_late, up_late, matrices = gate_up_a(
            rank_word, gain_parts, *weights, *(half for k in early for half in slices[k])
        )
        hidden = gate_up_b(gain_parts, gate_late, up_late, gate, up, squares, *(half for k in late for half in slices[k]))
        hidden, also = lax.optimization_barrier((hidden, also))
        hiddens = {k: shifted(hidden, "tensor", k) for k in RANK_SHIFTS}
        hiddens[0] = hidden
        total = down_a(matrices, *(hiddens[k] for k in order[:1]))
        outs = down_b(matrices, total, *(hiddens[k] for k in order[1:]))
        blocks_out = [k for pair in BLOCK_PAIRS for k in pair]
        return [outs[blocks_out.index(k)] for k in range(chips)], also

    def to_home(blocks):
        back = {k: shifted(blocks[k], "expert", groups - 2 * k) for k in CHIP_SHIFTS}
        back[0] = blocks[0]
        return [back[k] for k in range(chips)]

    def combined(stream, blocks, which):
        update, swapped = combine(which.reshape(1), high, low, *blocks)
        return (stream.astype(f32) + (update + core_swap(swapped).astype(f32))).astype(bf16)

    def kept(collected, fresh, spot):
        own = lax.dynamic_slice_in_dim(fresh, core * local_tokens, local_tokens)[None]
        held = lax.dynamic_slice_in_dim(collected, jnp.minimum(spot, micro_count - 1), 1)
        own = jnp.where(spot < micro_count, own, held)
        return lax.dynamic_update_slice_in_dim(collected, own, jnp.minimum(spot, micro_count - 1), 0)

    outgoing = dispatch(jnp.zeros(1, i32), first_place, entering[0])
    moved = {k: shifted(outgoing[k], "expert", 2 * k) for k in CHIP_SHIFTS}
    moved[0] = outgoing[0]

    next_info = shifted(info, "pipe", sections - 1)
    place = tables(where, next_info)[0]

    blocks, stream = expert_work([moved[k] for k in range(chips)], down_parts, entering[0], gain_parts)
    fresh = combined(stream, to_home(blocks), jnp.zeros((), i32))
    collected = kept(jnp.zeros((micro_count, local_tokens, width), bf16), fresh, 0)
    fresh = jnp.where(section == sections - 1, entering[1], fresh)

    def tick(index, carry):
        fresh, collected = carry
        unit = index - section
        leaving = jnp.where(section == sections - 1, 1, jnp.clip(unit - 1, 0, micro_count - 1))
        outgoing = dispatch(leaving.reshape(1), place, fresh)
        moved = {k: onward(outgoing[k], k) for k in (*CHIP_SHIFTS, 0)}
        stream = shifted(fresh, "pipe", 1)
        gains_here = marker(index.reshape(1), gain_parts)
        blocks, stream = expert_work([moved[k] for k in range(chips)], down_parts, stream, gains_here)
        fresh = combined(stream, to_home(blocks), jnp.clip(unit, 0, micro_count - 1))
        return fresh, kept(collected, fresh, jnp.clip(unit, 0, micro_count))

    fresh, collected = lax.fori_loop(1, micro_count + sections - 1, tick, (fresh, collected))
    return collected[None]


def solution(mesh):
    return jax.shard_map(
        local,
        mesh=mesh,
        in_specs=(
            P(None, "expert", None),
            P("pipe", None),
            P("pipe", None, "expert", None),
            P("pipe", None, "expert", None),
            P("pipe", None, "expert", None),
            P("pipe", "expert", None, "tensor"),
            P("pipe", "expert", None, "tensor"),
            P("pipe", "expert", "tensor", None),
        ),
        out_specs=P("pipe", None, "expert", "tensor"),
        check_vma=False,
    )
```
